256 devices in a mesh: freq: 32 (over z, x), rcv: 8 (over y, core).
Axes of the slice: x: 4, y: 4, z: 8, core: 2. Of those that a mesh axis runs over, the one named last changes fastest.
Arguments:
- primaries_start: float32 [512, 1024, 128], P(('rcv', 'freq')), may hold values from -6 to 6
- surface_operator: bfloat16 [512, 2, 384, 512], P('freq', None, 'rcv'), may hold values from -0.25 to 0.25
- data_spectra: bfloat16 [384, 512, 2, 128], P('rcv', 'freq'), may hold values from -6 to 6
- shrinkage: float32 [128], replicated, may hold values from 0.2 to 2
Outputs:
- primaries: float32 [512, 1024, 128], P(('rcv', 'freq'))
- residual_spectra: bfloat16 [384, 512, 2, 128], P('rcv', 'freq')
The draws below stay inside these ranges and needn't reach their ends.
All inputs are finite; a program needn't handle non-finite values.
Results may differ from the reference program's by a relative error of at most 0.0085.
Values may be sent and summed in bfloat16 or wider, within the bound.
No kernel may reach another device: no remote copies, remote signals or barrier semaphores. Data moves between devices by JAX's collectives and lax.ppermute only.
A program may use at most 64 MiB of HBM per device.

```python
import math
import jax
import jax.numpy as jnp
from jax import lax

S = 128
NS = 512
R = 384
T_SIZE = 1024
ITERS = 2
NF = 512


def strengthened(drawn, key, source, target, shards_of, factor):
    owner, partner = [(jnp.arange(drawn.shape[position]) // (drawn.shape[position] // shards_of)).reshape([-1 if axis == position else 1 for axis in range(drawn.ndim)]) for position in (source, target)]
    chosen = jax.random.permutation(key, shards_of)[partner]
    strong = (owner == chosen) | (owner == (partner + shards_of // 2) % shards_of)
    return jnp.where(strong, factor * drawn, drawn)


def block_scale(own_key, dims, pieces, least, top_value):
    factor_of = 1.0
    for dim, parts in pieces:
        steps = jax.random.uniform(jax.random.fold_in(jax.random.fold_in(own_key, 6), dim), (parts,), jnp.float32, least / len(pieces), top_value / len(pieces))
        factor_of = factor_of * jnp.repeat(jnp.exp(steps), dims[dim] // parts).reshape((-1,) + (1,) * (len(dims) - 1 - dim))
    return factor_of


def centred(stream_key, extent, deviation, limit, cuts=(), held_as=jnp.bfloat16):
    array = deviation * jax.random.normal(stream_key, extent, jnp.float32)
    if cuts:
        array = array * block_scale(stream_key, extent, cuts, -0.22, 0.18)
    return jnp.clip(array, -limit, limit).astype(held_as)


def heavy_noise(stream_key, dims, width, limit, shards, heavy, kind=jnp.bfloat16):
    values = width * jax.random.normal(stream_key, dims, jnp.float32)
    if shards:
        values = values * block_scale(stream_key, dims, shards, -0.22, 0.18)
    return jnp.clip(strengthened(values, jax.random.fold_in(stream_key, 3), *heavy), -limit, limit).astype(kind)


def setup_inputs(seed: int = 0) -> dict:
    key_of = jax.random.split(jax.random.key(seed), 5)
    primaries_start = centred(key_of[0], (NS, T_SIZE, S), 1.0, 6.0, ((0, 256),), jnp.float32)
    surface_operator = heavy_noise(key_of[1], (NF, 2, R, NS), (2 * NS) ** -0.5, 0.25, ((0, 32), (2, 8)), (2, 3, 8, 2.0))
    data_spectra = centred(key_of[2], (R, NF, 2, S), 1.0, 6.0, ((0, 8), (1, 32)))
    shrinkage = jnp.clip(jnp.exp(jax.random.uniform(key_of[3], (S,), jnp.float32, math.log(0.2), math.log(2.0))), 0.2, 2.0)
    return dict(primaries_start=primaries_start, surface_operator=surface_operator, data_spectra=data_spectra, shrinkage=shrinkage)


def transform_table(frequencies, samples):
    freq_index = jnp.arange(frequencies, dtype=jnp.int32)[:, None]
    sample_index = jnp.arange(samples, dtype=jnp.int32)[None, :]
    phase = freq_index * sample_index % samples
    angle = phase.astype(jnp.float32) * (2.0 * math.pi / samples)
    factor = math.sqrt(2.0 / samples)
    return jnp.stack([factor * jnp.cos(angle), -factor * jnp.sin(angle)], axis=1).astype(jnp.bfloat16)

def widen(values):
    return lax.optimization_barrier(values.astype(jnp.bfloat16)).astype(jnp.float32)

def one_frequency(items):
    operator, spectrum, recorded = items
    real_op = operator[0]
    imag_op = operator[1]
    real_in = spectrum[:, 0]
    imag_in = spectrum[:, 1]
    real_out = jnp.dot(real_op, real_in, preferred_element_type=jnp.float32) - jnp.dot(imag_op, imag_in, preferred_element_type=jnp.float32)
    imag_out = jnp.dot(real_op, imag_in, preferred_element_type=jnp.float32) + jnp.dot(imag_op, real_in, preferred_element_type=jnp.float32)
    resid = (recorded.astype(jnp.float32) - jnp.stack([real_out, imag_out], axis=1)).astype(jnp.bfloat16)
    real_res = resid[:, 0]
    imag_res = resid[:, 1]
    real_dir = jnp.dot(real_op.T, real_res, preferred_element_type=jnp.float32) + jnp.dot(imag_op.T, imag_res, preferred_element_type=jnp.float32)
    imag_dir = jnp.dot(real_op.T, imag_res, preferred_element_type=jnp.float32) - jnp.dot(imag_op.T, real_res, preferred_element_type=jnp.float32)
    return (resid, jnp.stack([real_dir, imag_dir], axis=1))

def reference(primaries_start, surface_operator, data_spectra, shrinkage):
    table = transform_table(NF, T_SIZE).astype(jnp.float32)
    primaries = primaries_start
    count_total = 2.0 * NF * NS * S
    residual = data_spectra
    for iteration in range(ITERS):
        spectra = jnp.einsum('kct,nts->nkcs', table, widen(primaries)).astype(jnp.bfloat16)
        residual_f, direction_f = lax.map(one_frequency, (surface_operator, jnp.moveaxis(spectra, 1, 0), jnp.moveaxis(data_spectra, 1, 0)))
        residual = jnp.moveaxis(residual_f, 0, 1)
        direction = jnp.moveaxis(direction_f, 0, 1)
        residual_norm = jnp.sum(jnp.square(residual.astype(jnp.float32)))
        direction_norm = jnp.sum(jnp.square(direction))
        step_size = 0.5 * residual_norm / (direction_norm + 1e-06)
        threshold = shrinkage[None, None, :] * (step_size * jnp.sqrt(direction_norm / count_total))
        update = jnp.einsum('kct,nkcs->nts', table, widen(direction))
        moved = primaries + step_size * update
        primaries = moved - jnp.clip(moved, -threshold, threshold)
    return (primaries, residual)
```

```python
import math

import jax
import jax.numpy as jnp
import numpy as np
from jax import lax
from jax.sharding import PartitionSpec as P

S = 128
NS = 512
R = 384
T_SIZE = 1024
ITERS = 2
NF = 512
ALL = ("rcv", "freq")


def transform_table(freq_parts, rcv_parts):
    freq_index = np.arange(NF).reshape(freq_parts, rcv_parts, -1).transpose(1, 0, 2).reshape(-1, 1)
    phase = freq_index * np.arange(T_SIZE)[None, :] % T_SIZE
    angle = phase * (2.0 * math.pi / T_SIZE)
    factor = math.sqrt(2.0 / T_SIZE)
    table = np.stack([factor * np.cos(angle), -factor * np.sin(angle)], axis=1)
    return jnp.asarray(table.reshape(2 * NF, T_SIZE).astype(np.float32)).astype(jnp.bfloat16)


def split_three(value):
    high = lax.reduce_precision(value, 8, 7)
    rest = value - high
    middle = lax.reduce_precision(rest, 8, 7)
    return jnp.stack([high, middle, rest - middle])


def forward(op, points):
    def product(left, right):
        return jnp.einsum("akrn,nks->arks", left, right, preferred_element_type=jnp.float32)

    real_op, imag_op = op[:, :, 0], op[:, :, 1]
    real_in, imag_in = points[:, :, 0], points[:, :, 1]
    real_out = product(real_op, real_in) - product(imag_op, imag_in)
    imag_out = product(real_op, imag_in) + product(imag_op, real_in)
    return jnp.stack([real_out, imag_out], axis=3)


def adjoint(op, resid):
    def product(left, right):
        return jnp.einsum("akrn,arks->nks", left, right, preferred_element_type=jnp.float32)

    real_op, imag_op = op[:, :, 0], op[:, :, 1]
    real_res, imag_res = resid[:, :, :, 0], resid[:, :, :, 1]
    real_dir = product(real_op, real_res) + product(imag_op, imag_res)
    imag_dir = product(real_op, imag_res) - product(imag_op, real_res)
    return jnp.stack([real_dir, imag_dir], axis=2)


def local(freq_parts, rcv_parts, primaries_start, surface_operator, data_spectra, shrinkage):
    devices = freq_parts * rcv_parts
    own_n = NS // devices
    own_k = NF // devices
    rows = R // rcv_parts
    table = transform_table(freq_parts, rcv_parts)
    op = lax.all_to_all(surface_operator, "rcv", split_axis=0, concat_axis=0, tiled=True)
    op = op.reshape(rcv_parts, own_k, 2, rows, NS)
    data = lax.all_to_all(data_spectra, "rcv", split_axis=1, concat_axis=0, tiled=True)
    data = data.reshape(rcv_parts, rows, own_k, 2, S).astype(jnp.float32)
    primaries = primaries_start
    count_total = 2.0 * NF * NS * S
    residual = None
    for iteration in range(ITERS):
        spectra = jnp.einsum(
            "kt,nts->kns", table, primaries.astype(jnp.bfloat16), preferred_element_type=jnp.float32
        ).astype(jnp.bfloat16)
        spectra = spectra.reshape(devices, own_k, 2, own_n, S).transpose(0, 3, 1, 2, 4)
        points = lax.all_to_all(spectra, ALL, split_axis=0, concat_axis=0, tiled=True)
        points = points.reshape(NS, own_k, 2, S)
        residual = (data - forward(op, points)).astype(jnp.bfloat16)
        direction = adjoint(op, residual)
        residual_sq = jnp.sum(jnp.square(residual.astype(jnp.float32)))
        direction_sq = jnp.sum(jnp.square(direction))
        sums = jnp.concatenate([split_three(residual_sq), split_three(direction_sq)])
        sums = jnp.pad(sums.astype(jnp.bfloat16), (0, 2 * S - 6)).reshape(1, 1, 2, S)
        low = direction.astype(jnp.bfloat16).reshape(devices, own_n * own_k, 2, S)
        packed = jnp.concatenate([low, jnp.broadcast_to(sums, (devices, 1, 2, S))], axis=1)
        packed = lax.all_to_all(packed, ALL, split_axis=0, concat_axis=0, tiled=True)
        totals = jnp.sum(packed[:, -1, 0, :6].astype(jnp.float32), axis=0)
        residual_norm = jnp.sum(totals[:3])
        direction_norm = jnp.sum(totals[3:])
        step_size = 0.5 * residual_norm / (direction_norm + 1e-06)
        threshold = shrinkage[None, None, :] * (step_size * jnp.sqrt(direction_norm / count_total))
        own = packed[:, :-1].reshape(devices, own_n, own_k, 2, S).transpose(1, 0, 2, 3, 4)
        update = jnp.einsum(
            "kt,nks->nts",
            table,
            own.reshape(own_n, 2 * NF, S),
            preferred_element_type=jnp.float32,
        )
        moved = primaries + step_size * update
        primaries = moved - jnp.clip(moved, -threshold, threshold)
    residual = residual.reshape(R, own_k, 2, S)
    residual = lax.all_to_all(residual, "rcv", split_axis=0, concat_axis=1, tiled=True)
    return (primaries, residual)


def solution(mesh):
    freq_parts, rcv_parts = mesh.shape["freq"], mesh.shape["rcv"]

    def body(*args):
        return local(freq_parts, rcv_parts, *args)

    return jax.shard_map(
        body,
        mesh=mesh,
        in_specs=(
            P(("rcv", "freq"), None, None),
            P("freq", None, "rcv", None),
            P("rcv", "freq", None, None),
            P(),
        ),
        out_specs=(P(("rcv", "freq"), None, None), P("rcv", "freq", None, None)),
        check_vma=False,
    )
```

```python
import functools
import math

import jax
import jax.numpy as jnp
import numpy as np
from jax import lax
from jax.experimental import pallas as pl
from jax.experimental.pallas import tpu as pltpu
from jax.sharding import PartitionSpec as P

S = 128
NS = 512
R = 384
T_SIZE = 1024
ITERS = 2
NF = 512
ALL = ("rcv", "freq")
PARTS = 4
WIDE = PARTS + 1


def transform_table(freq_parts, rcv_parts):
    freq_index = np.arange(NF).reshape(freq_parts, rcv_parts, -1).transpose(2, 1, 0).reshape(-1, 1, freq_parts * rcv_parts, 1)
    phase = freq_index * np.arange(T_SIZE) % T_SIZE
    angle = phase * (2.0 * math.pi / T_SIZE)
    factor = math.sqrt(2.0 / T_SIZE)
    table = np.concatenate([factor * np.cos(angle), -factor * np.sin(angle)], axis=1)
    return jnp.asarray(table.reshape(2 * NF, T_SIZE).astype(np.float32)).astype(jnp.bfloat16)


def call(kernel, out_shape, scratch, inputs, flops):
    return pl.pallas_call(
        kernel,
        out_shape=out_shape,
        in_specs=[pl.BlockSpec(memory_space=pltpu.VMEM)] * len(inputs),
        out_specs=jax.tree.map(lambda _: pl.BlockSpec(memory_space=pltpu.VMEM), out_shape),
        scratch_shapes=[pltpu.VMEM(shape, jnp.float32) for shape in scratch],
        compiler_params=pltpu.CompilerParams(vmem_limit_bytes=32 * 2**20),
        cost_estimate=pl.CostEstimate(flops=flops, bytes_accessed=4 * 2**20, transcendentals=0),
    )(*inputs)


def transform(table_ref, low, rows_ref, spectra_ref, owners):
    for part in range(PARTS):
        block = jnp.dot(table_ref[pl.ds(part * owners, owners), :], low, preferred_element_type=jnp.float32)
        for point in range(2):
            rows_ref[pl.ds(point * PARTS + part, owners, stride=2 * PARTS), :] = block[:, point * S:(point + 1) * S]
    spectra_ref[...] = rows_ref[...].astype(jnp.bfloat16)


def start_kernel(owners, primaries_ref, table_ref, spectra_ref, rows_ref):
    low = jnp.concatenate([primaries_ref[0].astype(jnp.bfloat16), primaries_ref[1].astype(jnp.bfloat16)], axis=1)
    transform(table_ref, low, rows_ref, spectra_ref, owners)


def split_three(value):
    high = value.astype(jnp.bfloat16).astype(jnp.float32)
    rest = value - high
    middle = rest.astype(jnp.bfloat16).astype(jnp.float32)
    return [high, middle, rest - middle]


def physics_kernel(blocks, points_ref, op_ref, data_ref, packed_ref, residual_ref, rows_ref, wide_ref):
    rows = op_ref.shape[2]
    rows_ref[...] = points_ref[...].astype(jnp.float32)
    residual_sq = jnp.zeros((1, 1), jnp.float32)
    direction_sq = jnp.zeros((1, 1), jnp.float32)
    for k in range(2):
        spectra = jnp.concatenate(
            [rows_ref[pl.ds(2 * k + c, NS, stride=PARTS), :].astype(jnp.bfloat16) for c in range(2)], axis=1
        )
        op = jnp.concatenate([op_ref[2 * a + k].reshape(2 * rows, NS) for a in range(blocks)], axis=0)
        product = jnp.dot(op, spectra, preferred_element_type=jnp.float32).reshape(blocks, 2, rows, 2 * S)
        stacked = []
        for a in range(blocks):
            real = product[a, 0, :, :S] - product[a, 1, :, S:]
            imag = product[a, 0, :, S:] + product[a, 1, :, :S]
            real = (data_ref[2 * a + k, 0].astype(jnp.float32) - real).astype(jnp.bfloat16)
            imag = (data_ref[2 * a + k, 1].astype(jnp.float32) - imag).astype(jnp.bfloat16)
            residual_ref[2 * a + k, 0] = real
            residual_ref[2 * a + k, 1] = imag
            wide_real = real.astype(jnp.float32)
            wide_imag = imag.astype(jnp.float32)
            residual_sq += jnp.sum(wide_real * wide_real + wide_imag * wide_imag, keepdims=True)
            stacked.append(jnp.concatenate([real, imag], axis=1))
            stacked.append(jnp.concatenate([imag, -real], axis=1))
        direction = lax.dot_general(
            op, jnp.concatenate(stacked, axis=0), (((0,), (0,)), ((), ())), preferred_element_type=jnp.float32
        )
        direction_sq += jnp.sum(direction * direction, keepdims=True)
        for c in range(2):
            wide_ref[pl.ds(2 * k + c, NS, stride=WIDE), :] = direction[:, c * S:(c + 1) * S]
    lane = lax.broadcasted_iota(jnp.int32, (8, S), 1)
    sums = jnp.zeros((8, S), jnp.float32)
    for place, piece in enumerate(split_three(residual_sq) + split_three(direction_sq)):
        sums = jnp.where(lane == place, piece, sums)
    wide_ref[pl.ds(PARTS, NS, stride=WIDE), :] = jnp.broadcast_to(sums[:1], (NS, S))
    packed_ref[...] = wide_ref[...].astype(jnp.bfloat16)


def update(owners, packed_ref, table_ref, primaries_ref, shrinkage_ref, wide_ref, new_ref):
    wide_ref[...] = packed_ref[...].astype(jnp.float32)
    totals = jnp.sum(wide_ref[pl.ds(PARTS, owners, stride=2 * WIDE), :], axis=0, keepdims=True)
    lane = lax.broadcasted_iota(jnp.int32, (1, S), 1)
    residual_norm = jnp.sum(jnp.where(lane < 3, totals, 0.0), axis=1, keepdims=True)
    direction_norm = jnp.sum(jnp.where((lane >= 3) & (lane < 6), totals, 0.0), axis=1, keepdims=True)
    step_size = 0.5 * residual_norm / (direction_norm + 1e-06)
    threshold = shrinkage_ref[...] * (step_size * jnp.sqrt(direction_norm / (2.0 * NF * NS * S)))
    sides = []
    for point in range(2):
        pieces = [
            wide_ref[pl.ds(point * WIDE + part, owners, stride=2 * WIDE), :].astype(jnp.bfloat16)
            for part in range(PARTS)
        ]
        sides.append(jnp.concatenate(pieces, axis=0))
    direction = jnp.concatenate(sides, axis=1)
    lows = []
    block = 256
    for start in range(0, T_SIZE, block):
        change = lax.dot_general(
            table_ref[:, pl.ds(start, block)], direction, (((0,), (0,)), ((), ())), preferred_element_type=jnp.float32
        )
        halves = []
        for point in range(2):
            moved = primaries_ref[point, pl.ds(start, block), :] + step_size * change[:, point * S:(point + 1) * S]
            new = moved - jnp.clip(moved, -threshold, threshold)
            new_ref[point, pl.ds(start, block), :] = new
            halves.append(new.astype(jnp.bfloat16))
        lows.append(jnp.concatenate(halves, axis=1))
    return lows


def middle_kernel(owners, packed_ref, table_ref, primaries_ref, shrinkage_ref, new_ref, spectra_ref, wide_ref, rows_ref):
    lows = update(owners, packed_ref, table_ref, primaries_ref, shrinkage_ref, wide_ref, new_ref)
    transform(table_ref, jnp.concatenate(lows, axis=0), rows_ref, spectra_ref, owners)


def last_kernel(owners, packed_ref, table_ref, primaries_ref, shrinkage_ref, new_ref, wide_ref):
    update(owners, packed_ref, table_ref, primaries_ref, shrinkage_ref, wide_ref, new_ref)


def exchange(array, devices, scope):
    with jax.named_scope(scope):
        pairs = array.reshape(devices, array.shape[0] // (2 * devices), 2, S)
        return lax.all_to_all(pairs, ALL, split_axis=0, concat_axis=0, tiled=True).reshape(array.shape)


def local(freq_parts, rcv_parts, primaries_start, surface_operator, data_spectra, shrinkage):
    devices = freq_parts * rcv_parts
    rows = R // rcv_parts
    half, wide = (devices * 2 * PARTS, S), (devices * 2 * WIDE, S)
    bf16, f32 = jnp.bfloat16, jnp.float32
    table = transform_table(freq_parts, rcv_parts)
    shrinkage = shrinkage.reshape(1, S)
    with jax.named_scope("operator"):
        op = lax.all_to_all(surface_operator, "rcv", split_axis=0, concat_axis=0, tiled=True)
    with jax.named_scope("recorded"):
        data = lax.all_to_all(data_spectra.transpose(1, 2, 0, 3), "rcv", split_axis=0, concat_axis=0, tiled=True)
    primaries = primaries_start
    spectra = call(
        functools.partial(start_kernel, devices),
        jax.ShapeDtypeStruct(half, bf16),
        [half],
        (primaries, table),
        2 * 1024 * 1024 * 256,
    )
    for iteration in range(ITERS):
        points = exchange(spectra, devices, f"spectra{iteration}")
        packed, residual = call(
            functools.partial(physics_kernel, rcv_parts),
            (jax.ShapeDtypeStruct(wide, bf16), jax.ShapeDtypeStruct((2 * rcv_parts, 2, rows, S), bf16)),
            [half, wide],
            (points, op, data),
            4 * 2 * 768 * 512 * 256,
        )
        packed = exchange(packed, devices, f"direction{iteration}")
        shape = jax.ShapeDtypeStruct(primaries.shape, f32)
        inputs = (packed, table, primaries, shrinkage)
        if iteration + 1 < ITERS:
            primaries, spectra = call(
                functools.partial(middle_kernel, devices),
                (shape, jax.ShapeDtypeStruct(half, bf16)),
                [wide, half],
                inputs,
                4 * 1024 * 1024 * 256,
            )
        else:
            primaries = call(functools.partial(last_kernel, devices), shape, [wide], inputs, 2 * 1024 * 1024 * 256)
    with jax.named_scope("returned"):
        residual = lax.all_to_all(residual, "rcv", split_axis=0, concat_axis=0, tiled=True)
    return (primaries, residual.transpose(2, 0, 1, 3))


def solution(mesh):
    freq_parts, rcv_parts = mesh.shape["freq"], mesh.shape["rcv"]

    def body(*args):
        return local(freq_parts, rcv_parts, *args)

    return jax.shard_map(
        body,
        mesh=mesh,
        in_specs=(
            P(("rcv", "freq"), None, None),
            P("freq", None, "rcv", None),
            P("rcv", "freq", None, None),
            P(),
        ),
        out_specs=(P(("rcv", "freq"), None, None), P("rcv", "freq", None, None)),
        check_vma=False,
    )
```

```python
import functools
import math

import jax
import jax.numpy as jnp
import numpy as np
from jax import lax
from jax.experimental import pallas as pl
from jax.experimental.pallas import tpu as pltpu
from jax.sharding import PartitionSpec as P


S = 128
NS = 512
R = 384
T_SIZE = 1024
ITERS = 2
NF = 512
ALL = ("rcv", "freq")
LANES = 128
PARTS = 4
WIDE = PARTS + 1


def table_base(freq_parts, rcv_parts):
    freq_index = np.arange(NF).reshape(freq_parts, rcv_parts, -1).transpose(2, 1, 0).reshape(-1, 1)
    angle = freq_index * np.arange(LANES) % T_SIZE * (2.0 * math.pi / T_SIZE)
    factor = math.sqrt(2.0 / T_SIZE)
    return jnp.asarray(np.stack([factor * np.cos(angle), factor * np.sin(angle)]).astype(np.float32))


def fill_table(base_ref, table_ref, owners, rcv_parts):
    run = owners // rcv_parts
    for place in range(2):
        for owner in range(rcv_parts):
            rows = pl.ds(place * owners + owner * run, run)
            cosine, sine = base_ref[0, rows, :], base_ref[1, rows, :]
            for tile in range(T_SIZE // LANES):
                turn = math.pi / 4 * ((2 * owner + place) * tile % 8)
                cos, sin = round(math.cos(turn), 12), round(math.sin(turn), 12)
                columns = pl.ds(tile * LANES, LANES)
                real = cosine * cos - sine * sin
                imag = -(sine * cos + cosine * sin)
                for part, value in ((0, real), (1, imag)):
                    table_ref[pl.ds((2 * place + part) * owners + owner * run, run), columns] = value.astype(jnp.bfloat16)


def call(kernel, out_shape, scratch, inputs, flops, spaces=None):
    return pl.pallas_call(
        kernel,
        out_shape=out_shape,
        in_specs=[pl.BlockSpec(memory_space=space) for space in spaces or [pltpu.VMEM] * len(inputs)],
        out_specs=jax.tree.map(lambda _: pl.BlockSpec(memory_space=pltpu.VMEM), out_shape),
        scratch_shapes=scratch,
        compiler_params=pltpu.CompilerParams(vmem_limit_bytes=32 * 2**20),
        cost_estimate=pl.CostEstimate(flops=flops, bytes_accessed=4 * 2**20, transcendentals=0),
    )(*inputs)


def transform(table_ref, low, rows_ref, spectra_ref, owners):
    for part in range(PARTS):
        block = jnp.dot(table_ref[pl.ds(part * owners, owners), :], low, preferred_element_type=jnp.float32)
        for point in range(2):
            rows_ref[pl.ds(point * PARTS + part, owners, stride=2 * PARTS), :] = block[:, point * S:(point + 1) * S]
    spectra_ref[...] = rows_ref[...].astype(jnp.bfloat16)


def start_kernel(owners, rcv_parts, primaries_ref, base_ref, spectra_ref, rows_ref, table_ref):
    fill_table(base_ref, table_ref, owners, rcv_parts)
    low = jnp.concatenate([primaries_ref[0].astype(jnp.bfloat16), primaries_ref[1].astype(jnp.bfloat16)], axis=1)
    transform(table_ref, low, rows_ref, spectra_ref, owners)


def split_three(value):
    high = value.astype(jnp.bfloat16).astype(jnp.float32)
    rest = value - high
    middle = rest.astype(jnp.bfloat16).astype(jnp.float32)
    return [high, middle, rest - middle]


def physics_kernel(blocks, returned, points_ref, *refs):
    sources, data_refs = refs[:blocks], refs[blocks:2 * blocks]
    packed_ref = refs[2 * blocks]
    residual_refs = refs[2 * blocks + 1:2 * blocks + 1 + returned]
    op_ref, rows_ref, wide_ref, sem = refs[2 * blocks + 1 + returned:]
    rows = op_ref.shape[3]
    copies = [pltpu.make_async_copy(source, op_ref.at[a], sem.at[a]) for a, source in enumerate(sources)]
    for copy in copies:
        copy.start()
    rows_ref[...] = points_ref[...].astype(jnp.float32)
    for copy in copies:
        copy.wait()
    residual_sq = jnp.zeros((1, 1), jnp.float32)
    direction_sq = jnp.zeros((1, 1), jnp.float32)
    for k in range(2):
        spectra = jnp.concatenate(
            [rows_ref[pl.ds(2 * k + c, NS, stride=PARTS), :].astype(jnp.bfloat16) for c in range(2)], axis=1
        )
        op = jnp.concatenate([op_ref[a, k].reshape(2 * rows, NS) for a in range(blocks)], axis=0)
        product = jnp.dot(op, spectra, preferred_element_type=jnp.float32).reshape(blocks, 2, rows, 2 * S)
        stacked = []
        for a in range(blocks):
            real = product[a, 0, :, :S] - product[a, 1, :, S:]
            imag = product[a, 0, :, S:] + product[a, 1, :, :S]
            real = (data_refs[a][k, 0].astype(jnp.float32) - real).astype(jnp.bfloat16)
            imag = (data_refs[a][k, 1].astype(jnp.float32) - imag).astype(jnp.bfloat16)
            if returned:
                residual_refs[a][k, 0] = real
                residual_refs[a][k, 1] = imag
            wide_real = real.astype(jnp.float32)
            wide_imag = imag.astype(jnp.float32)
            residual_sq += jnp.sum(wide_real * wide_real + wide_imag * wide_imag, keepdims=True)
            stacked.append(jnp.concatenate([real, imag], axis=1))
            stacked.append(jnp.concatenate([imag, -real], axis=1))
        direction = lax.dot_general(
            op, jnp.concatenate(stacked, axis=0), (((0,), (0,)), ((), ())), preferred_element_type=jnp.float32
        )
        direction_sq += jnp.sum(direction * direction, keepdims=True)
        for c in range(2):
            wide_ref[pl.ds(2 * k + c, NS, stride=WIDE), :] = direction[:, c * S:(c + 1) * S]
    lane = lax.broadcasted_iota(jnp.int32, (8, S), 1)
    sums = jnp.zeros((8, S), jnp.float32)
    for place, piece in enumerate(split_three(residual_sq) + split_three(direction_sq)):
        sums = jnp.where(lane == place, piece, sums)
    wide_ref[pl.ds(PARTS, NS, stride=WIDE), :] = jnp.broadcast_to(sums[:1], (NS, S))
    packed_ref[...] = wide_ref[...].astype(jnp.bfloat16)


def update(owners, packed_ref, table_ref, primaries_ref, shrinkage_ref, wide_ref, new_ref):
    wide_ref[...] = packed_ref[...].astype(jnp.float32)
    totals = jnp.sum(wide_ref[pl.ds(PARTS, owners, stride=2 * WIDE), :], axis=0, keepdims=True)
    lane = lax.broadcasted_iota(jnp.int32, (1, S), 1)
    residual_norm = jnp.sum(jnp.where(lane < 3, totals, 0.0), axis=1, keepdims=True)
    direction_norm = jnp.sum(jnp.where((lane >= 3) & (lane < 6), totals, 0.0), axis=1, keepdims=True)
    step_size = 0.5 * residual_norm / (direction_norm + 1e-06)
    threshold = shrinkage_ref[...] * (step_size * jnp.sqrt(direction_norm / (2.0 * NF * NS * S)))
    sides = []
    for point in range(2):
        pieces = [
            wide_ref[pl.ds(point * WIDE + part, owners, stride=2 * WIDE), :].astype(jnp.bfloat16)
            for part in range(PARTS)
        ]
        sides.append(jnp.concatenate(pieces, axis=0))
    direction = jnp.concatenate(sides, axis=1)
    lows = []
    block = 256
    for start in range(0, T_SIZE, block):
        change = lax.dot_general(
            table_ref[:, pl.ds(start, block)], direction, (((0,), (0,)), ((), ())), preferred_element_type=jnp.float32
        )
        halves = []
        for point in range(2):
            moved = primaries_ref[point, pl.ds(start, block), :] + step_size * change[:, point * S:(point + 1) * S]
            new = moved - jnp.clip(moved, -threshold, threshold)
            new_ref[point, pl.ds(start, block), :] = new
            halves.append(new.astype(jnp.bfloat16))
        lows.append(jnp.concatenate(halves, axis=1))
    return lows


def middle_kernel(owners, rcv_parts, packed_ref, base_ref, primaries_ref, shrinkage_ref, new_ref, spectra_ref, wide_ref, table_ref, rows_ref):
    fill_table(base_ref, table_ref, owners, rcv_parts)
    lows = update(owners, packed_ref, table_ref, primaries_ref, shrinkage_ref, wide_ref, new_ref)
    transform(table_ref, jnp.concatenate(lows, axis=0), rows_ref, spectra_ref, owners)


def last_kernel(owners, rcv_parts, packed_ref, base_ref, primaries_ref, shrinkage_ref, new_ref, wide_ref, table_ref):
    fill_table(base_ref, table_ref, owners, rcv_parts)
    update(owners, packed_ref, table_ref, primaries_ref, shrinkage_ref, wide_ref, new_ref)


def split_kernel(blocks, me_ref, whole_ref, *refs):
    pieces, sem = refs[:blocks], refs[blocks]
    copies = [
        pltpu.make_async_copy(whole_ref.at[pl.ds(2 * (me_ref[0] ^ place), 2)], piece, sem.at[place])
        for place, piece in enumerate(pieces)
    ]
    for copy in copies:
        copy.start()
    for copy in copies:
        copy.wait()


def split(whole, me, blocks, space):
    piece = jax.ShapeDtypeStruct((2,) + whole.shape[1:], whole.dtype)
    return pl.pallas_call(
        functools.partial(split_kernel, blocks),
        out_shape=[piece] * blocks,
        in_specs=[pl.BlockSpec(memory_space=pltpu.SMEM), pl.BlockSpec(memory_space=pl.ANY)],
        out_specs=[pl.BlockSpec(memory_space=space)] * blocks,
        scratch_shapes=[pltpu.SemaphoreType.DMA((blocks,))],
        compiler_params=pltpu.CompilerParams(vmem_limit_bytes=8 * 2**20),
    )(me, whole)


def join_kernel(blocks, me_ref, *refs):
    pieces, whole_ref = refs[:blocks], refs[blocks]
    for place, piece in enumerate(pieces):
        whole_ref[pl.ds(2 * (me_ref[0] ^ place), 2)] = piece[...]


def join(pieces, me):
    blocks = len(pieces)
    shape = pieces[0].shape
    return pl.pallas_call(
        functools.partial(join_kernel, blocks),
        out_shape=jax.ShapeDtypeStruct((2 * blocks,) + shape[1:], pieces[0].dtype),
        in_specs=[pl.BlockSpec(memory_space=pltpu.SMEM)] + [pl.BlockSpec(memory_space=pltpu.VMEM)] * blocks,
        out_specs=pl.BlockSpec(memory_space=pltpu.VMEM),
        compiler_params=pltpu.CompilerParams(vmem_limit_bytes=8 * 2**20),
    )(me, *pieces)


def trade(pieces):
    blocks = len(pieces)
    return [pieces[0]] + [
        lax.ppermute(pieces[place], "rcv", [(source, source ^ place) for source in range(blocks)])
        for place in range(1, blocks)
    ]


def exchange(array, devices):
    pairs = array.reshape(devices, array.shape[0] // (2 * devices), 2, S)
    return lax.all_to_all(pairs, ALL, split_axis=0, concat_axis=0, tiled=True).reshape(array.shape)


def local(freq_parts, rcv_parts, primaries_start, surface_operator, data_spectra, shrinkage):
    devices = freq_parts * rcv_parts
    rows = R // rcv_parts
    half, wide = (devices * 2 * PARTS, S), (devices * 2 * WIDE, S)
    bf16, f32 = jnp.bfloat16, jnp.float32
    rows_half, rows_wide = pltpu.VMEM(half, f32), pltpu.VMEM(wide, f32)
    table = pltpu.VMEM((2 * NF, T_SIZE), bf16)
    base = table_base(freq_parts, rcv_parts)
    shrinkage = shrinkage.reshape(1, S)
    me = lax.axis_index("rcv").astype(jnp.int32).reshape(1)
    op = trade(split(surface_operator, me, rcv_parts, pl.ANY))
    data = trade(split(data_spectra.transpose(1, 2, 0, 3), me, rcv_parts, pltpu.VMEM))
    primaries = primaries_start
    spectra = call(
        functools.partial(start_kernel, devices, rcv_parts),
        jax.ShapeDtypeStruct(half, bf16),
        [rows_half, table],
        (primaries, base),
        2 * 1024 * 1024 * 256,
    )
    for iteration in range(ITERS):
        points = exchange(spectra, devices)
        returned = rcv_parts if iteration + 1 == ITERS else 0
        packed, *residual = call(
            functools.partial(physics_kernel, rcv_parts, returned),
            [jax.ShapeDtypeStruct(wide, bf16)] + [jax.ShapeDtypeStruct((2, 2, rows, S), bf16)] * returned,
            [
                pltpu.VMEM((rcv_parts, 2, 2, rows, NS), bf16),
                rows_half,
                rows_wide,
                pltpu.SemaphoreType.DMA((rcv_parts,)),
            ],
            (points, *op, *data),
            4 * 2 * 768 * 512 * 256,
            [pltpu.VMEM] + [pl.ANY] * rcv_parts + [pltpu.VMEM] * rcv_parts,
        )
        packed = exchange(packed, devices)
        shape = jax.ShapeDtypeStruct(primaries.shape, f32)
        inputs = (packed, base, primaries, shrinkage)
        if iteration + 1 < ITERS:
            primaries, spectra = call(
                functools.partial(middle_kernel, devices, rcv_parts),
                (shape, jax.ShapeDtypeStruct(half, bf16)),
                [rows_wide, table, rows_half],
                inputs,
                4 * 1024 * 1024 * 256,
            )
        else:
            primaries = call(functools.partial(last_kernel, devices, rcv_parts), shape, [rows_wide, table], inputs, 2 * 1024 * 1024 * 256)
    residual = join(trade(residual), me)
    return (primaries, residual.transpose(2, 0, 1, 3))


def solution(mesh):
    freq_parts, rcv_parts = mesh.shape["freq"], mesh.shape["rcv"]

    def body(*args):
        return local(freq_parts, rcv_parts, *args)

    return jax.shard_map(
        body,
        mesh=mesh,
        in_specs=(
            P(("rcv", "freq"), None, None),
            P("freq", None, "rcv", None),
            P("rcv", "freq", None, None),
            P(),
        ),
        out_specs=(P(("rcv", "freq"), None, None), P("rcv", "freq", None, None)),
        check_vma=False,
    )
```

```python
import functools
import math

import jax
import jax.numpy as jnp
import numpy as np
from jax import lax
from jax.experimental import pallas as pl
from jax.experimental.pallas import tpu as pltpu
from jax.sharding import PartitionSpec as P


S = 128
NS = 512
R = 384
T_SIZE = 1024
ITERS = 2
NF = 512
ALL = ("rcv", "freq")
LANES = 128
PARTS = 4
WIDE = PARTS + 1


def table_base(freq_parts, rcv_parts):
    freq_index = np.arange(NF).reshape(freq_parts, rcv_parts, -1).transpose(2, 1, 0).reshape(-1, 1)
    angle = freq_index * np.arange(LANES) % T_SIZE * (2.0 * math.pi / T_SIZE)
    factor = math.sqrt(2.0 / T_SIZE)
    return jnp.asarray(np.stack([factor * np.cos(angle), factor * np.sin(angle)]).astype(np.float32))


def fill_table(base_ref, table_ref, owners, rcv_parts):
    run = owners // rcv_parts
    for place in range(2):
        for owner in range(rcv_parts):
            rows = pl.ds(place * owners + owner * run, run)
            cosine, sine = base_ref[0, rows, :], base_ref[1, rows, :]
            for tile in range(T_SIZE // LANES):
                turn = math.pi / 4 * ((2 * owner + place) * tile % 8)
                cos, sin = round(math.cos(turn), 12), round(math.sin(turn), 12)
                columns = pl.ds(tile * LANES, LANES)
                real = cosine * cos - sine * sin
                imag = -(sine * cos + cosine * sin)
                for part, value in ((0, real), (1, imag)):
                    table_ref[pl.ds((2 * place + part) * owners + owner * run, run), columns] = value.astype(jnp.bfloat16)


def call(kernel, out_shape, scratch, inputs, flops, spaces=None, out_spaces=None):
    return pl.pallas_call(
        kernel,
        out_shape=out_shape,
        in_specs=[pl.BlockSpec(memory_space=space) for space in spaces or [pltpu.VMEM] * len(inputs)],
        out_specs=[pl.BlockSpec(memory_space=space) for space in out_spaces or [pltpu.VMEM] * len(out_shape)],
        scratch_shapes=scratch,
        compiler_params=pltpu.CompilerParams(vmem_limit_bytes=32 * 2**20),
        cost_estimate=pl.CostEstimate(flops=flops, bytes_accessed=4 * 2**20, transcendentals=0),
    )(*inputs)


def transform(table_ref, low, rows_ref, spectra_ref, owners):
    for part in range(PARTS):
        block = jnp.dot(table_ref[pl.ds(part * owners, owners), :], low, preferred_element_type=jnp.float32)
        for point in range(2):
            rows_ref[pl.ds(point * PARTS + part, owners, stride=2 * PARTS), :] = block[:, point * S:(point + 1) * S]
    spectra_ref[...] = rows_ref[...].astype(jnp.bfloat16)


def start_kernel(owners, blocks, me_ref, op_ref, primaries_ref, base_ref, *refs):
    pieces, spectra_ref = refs[:blocks], refs[blocks]
    held_ref, traces_ref, angles_ref, table_ref, rows_ref, sem = refs[blocks + 1:]
    targets = [pieces[0]] + [held_ref.at[place] for place in range(1, blocks)]
    fetch_base = pltpu.make_async_copy(base_ref, angles_ref, sem.at[2, 0])
    fetch_traces = pltpu.make_async_copy(primaries_ref, traces_ref, sem.at[2, 1])
    fetches = [
        pltpu.make_async_copy(op_ref.at[pl.ds(2 * (me_ref[0] ^ place), 2)], targets[place], sem.at[0, place])
        for place in range(blocks)
    ]
    stores = [pltpu.make_async_copy(targets[place], pieces[place], sem.at[1, place]) for place in range(1, blocks)]
    fetch_base.start()
    fetch_traces.start()
    for fetch in fetches:
        fetch.start()
    fetch_base.wait()
    fill_table(angles_ref, table_ref, owners, blocks)
    fetch_traces.wait()
    for place in range(blocks):
        fetches[place].wait()
        if place:
            stores[place - 1].start()
    low = jnp.concatenate([traces_ref[0].astype(jnp.bfloat16), traces_ref[1].astype(jnp.bfloat16)], axis=1)
    transform(table_ref, low, rows_ref, spectra_ref, owners)
    for store in stores:
        store.wait()


def split_three(value):
    high = value.astype(jnp.bfloat16).astype(jnp.float32)
    rest = value - high
    middle = rest.astype(jnp.bfloat16).astype(jnp.float32)
    return [high, middle, rest - middle]


def physics_kernel(blocks, returned, points_ref, *refs):
    op_refs, data_refs = refs[:blocks], refs[blocks:2 * blocks]
    packed_ref = refs[2 * blocks]
    returned_refs = refs[2 * blocks + 1:2 * blocks + 1 + returned]
    residual_ref, rows_ref, wide_ref, sem = refs[2 * blocks + 1 + returned:]
    rows = op_refs[0].shape[2]
    copies = []
    rows_ref[...] = points_ref[...].astype(jnp.float32)
    residual_sq = jnp.zeros((1, 1), jnp.float32)
    direction_sq = jnp.zeros((1, 1), jnp.float32)
    for k in range(2):
        spectra = jnp.concatenate(
            [rows_ref[pl.ds(2 * k + c, NS, stride=PARTS), :].astype(jnp.bfloat16) for c in range(2)], axis=1
        )
        op = jnp.concatenate([op_refs[a][k].reshape(2 * rows, NS) for a in range(blocks)], axis=0)
        product = jnp.dot(op, spectra, preferred_element_type=jnp.float32).reshape(blocks, 2, rows, 2 * S)
        stacked = []
        for a in range(blocks):
            real = product[a, 0, :, :S] - product[a, 1, :, S:]
            imag = product[a, 0, :, S:] + product[a, 1, :, :S]
            real = (data_refs[a][k, 0].astype(jnp.float32) - real).astype(jnp.bfloat16)
            imag = (data_refs[a][k, 1].astype(jnp.float32) - imag).astype(jnp.bfloat16)
            if returned:
                residual_ref[a, k, 0] = real
                residual_ref[a, k, 1] = imag
            wide_real = real.astype(jnp.float32)
            wide_imag = imag.astype(jnp.float32)
            residual_sq += jnp.sum(wide_real * wide_real + wide_imag * wide_imag, keepdims=True)
            stacked.append(jnp.concatenate([real, imag], axis=1))
            stacked.append(jnp.concatenate([imag, -real], axis=1))
        for a, out in enumerate(returned_refs):
            copies.append(pltpu.make_async_copy(residual_ref.at[a, k], out.at[k], sem.at[k, a]))
            copies[-1].start()
        direction = lax.dot_general(
            op, jnp.concatenate(stacked, axis=0), (((0,), (0,)), ((), ())), preferred_element_type=jnp.float32
        )
        direction_sq += jnp.sum(direction * direction, keepdims=True)
        for c in range(2):
            wide_ref[pl.ds(2 * k + c, NS, stride=WIDE), :] = direction[:, c * S:(c + 1) * S]
    lane = lax.broadcasted_iota(jnp.int32, (8, S), 1)
    sums = jnp.zeros((8, S), jnp.float32)
    for place, piece in enumerate(split_three(residual_sq) + split_three(direction_sq)):
        sums = jnp.where(lane == place, piece, sums)
    wide_ref[pl.ds(PARTS, NS, stride=WIDE), :] = jnp.broadcast_to(sums[:1], (NS, S))
    packed_ref[...] = wide_ref[...].astype(jnp.bfloat16)
    for copy in copies:
        copy.wait()


def update(owners, packed_ref, table_ref, primaries_ref, shrinkage_ref, wide_ref, held_ref, sem):
    fetch = pltpu.make_async_copy(primaries_ref, held_ref, sem.at[0])
    fetch.start()
    wide_ref[...] = packed_ref[...].astype(jnp.float32)
    totals = jnp.sum(wide_ref[pl.ds(PARTS, owners, stride=2 * WIDE), :], axis=0, keepdims=True)
    lane = lax.broadcasted_iota(jnp.int32, (1, S), 1)
    residual_norm = jnp.sum(jnp.where(lane < 3, totals, 0.0), axis=1, keepdims=True)
    direction_norm = jnp.sum(jnp.where((lane >= 3) & (lane < 6), totals, 0.0), axis=1, keepdims=True)
    step_size = 0.5 * residual_norm / (direction_norm + 1e-06)
    threshold = shrinkage_ref[...] * (step_size * jnp.sqrt(direction_norm / (2.0 * NF * NS * S)))
    sides = []
    for point in range(2):
        pieces = [
            wide_ref[pl.ds(point * WIDE + part, owners, stride=2 * WIDE), :].astype(jnp.bfloat16)
            for part in range(PARTS)
        ]
        sides.append(jnp.concatenate(pieces, axis=0))
    direction = jnp.concatenate(sides, axis=1)
    lows = []
    block = 256
    fetch.wait()
    for start in range(0, T_SIZE, block):
        change = lax.dot_general(
            table_ref[:, pl.ds(start, block)], direction, (((0,), (0,)), ((), ())), preferred_element_type=jnp.float32
        )
        halves = []
        for point in range(2):
            moved = held_ref[point, pl.ds(start, block), :] + step_size * change[:, point * S:(point + 1) * S]
            new = moved - jnp.clip(moved, -threshold, threshold)
            held_ref[point, pl.ds(start, block), :] = new
            halves.append(new.astype(jnp.bfloat16))
        lows.append(jnp.concatenate(halves, axis=1))
    return lows


def middle_kernel(owners, packed_ref, table_ref, primaries_ref, shrinkage_ref, new_ref, spectra_ref, *scratch):
    wide_ref, held_ref, rows_ref, sem = scratch
    lows = update(owners, packed_ref, table_ref, primaries_ref, shrinkage_ref, wide_ref, held_ref, sem)
    store = pltpu.make_async_copy(held_ref, new_ref, sem.at[1])
    store.start()
    transform(table_ref, jnp.concatenate(lows, axis=0), rows_ref, spectra_ref, owners)
    store.wait()


def last_kernel(owners, packed_ref, table_ref, primaries_ref, shrinkage_ref, new_ref, wide_ref, held_ref, sem):
    update(owners, packed_ref, table_ref, primaries_ref, shrinkage_ref, wide_ref, held_ref, sem)
    store = pltpu.make_async_copy(held_ref, new_ref, sem.at[1])
    store.start()
    store.wait()


def table_kernel(owners, rcv_parts, base_ref, first_ref, second_ref, table_ref, sem):
    fill_table(base_ref, table_ref, owners, rcv_parts)
    stores = [pltpu.make_async_copy(table_ref, whole, sem.at[i]) for i, whole in enumerate((first_ref, second_ref))]
    for store in stores:
        store.start()
    for store in stores:
        store.wait()


def pick_kernel(me_ref, whole_ref, *pieces):
    for place, piece in enumerate(pieces):
        piece[...] = whole_ref[pl.ds(2 * (me_ref[0] ^ place), 2)]


def pick(whole, me, blocks):
    shape = (2,) + whole.shape[1:]
    return pl.pallas_call(
        pick_kernel,
        out_shape=[jax.ShapeDtypeStruct(shape, whole.dtype)] * blocks,
        in_specs=[pl.BlockSpec(memory_space=pltpu.SMEM), pl.BlockSpec(memory_space=pltpu.VMEM)],
        out_specs=[pl.BlockSpec(memory_space=pltpu.VMEM)] * blocks,
        compiler_params=pltpu.CompilerParams(vmem_limit_bytes=8 * 2**20),
    )(me, whole)


def join_kernel(blocks, me_ref, *refs):
    pieces, whole_ref = refs[:blocks], refs[blocks]
    for place, piece in enumerate(pieces):
        whole_ref[pl.ds(2 * (me_ref[0] ^ place), 2)] = piece[...]


def join(pieces, me):
    blocks = len(pieces)
    shape = pieces[0].shape
    return pl.pallas_call(
        functools.partial(join_kernel, blocks),
        out_shape=jax.ShapeDtypeStruct((2 * blocks,) + shape[1:], pieces[0].dtype),
        in_specs=[pl.BlockSpec(memory_space=pltpu.SMEM)] + [pl.BlockSpec(memory_space=pltpu.VMEM)] * blocks,
        out_specs=pl.BlockSpec(memory_space=pltpu.VMEM),
        compiler_params=pltpu.CompilerParams(vmem_limit_bytes=8 * 2**20),
    )(me, *pieces)


def trade(pieces):
    blocks = len(pieces)
    traded = [pieces[0]]
    for place in range(1, blocks):
        traded.append(lax.ppermute(pieces[place], "rcv", [(source, source ^ place) for source in range(blocks)]))
    return traded


def exchange(array, devices):
    pairs = array.reshape(devices, array.shape[0] // (2 * devices), 2, S)
    return lax.all_to_all(pairs, ALL, split_axis=0, concat_axis=0, tiled=True).reshape(array.shape)


def local(freq_parts, rcv_parts, primaries_start, surface_operator, data_spectra, shrinkage):
    devices = freq_parts * rcv_parts
    rows = R // rcv_parts
    half, wide = (devices * 2 * PARTS, S), (devices * 2 * WIDE, S)
    bf16, f32 = jnp.bfloat16, jnp.float32
    rows_half, rows_wide = pltpu.VMEM(half, f32), pltpu.VMEM(wide, f32)
    table = pltpu.VMEM((2 * NF, T_SIZE), bf16)
    base = table_base(freq_parts, rcv_parts)
    shrinkage = shrinkage.reshape(1, S)
    me = lax.axis_index("rcv").astype(jnp.int32).reshape(1)
    data = trade(pick(data_spectra.transpose(1, 2, 0, 3), me, rcv_parts))
    primaries = primaries_start
    piece = (2, 2, rows, NS)
    *op, spectra = call(
        functools.partial(start_kernel, devices, rcv_parts),
        [jax.ShapeDtypeStruct(piece, bf16)]
        + [pltpu.HBM(piece, bf16)] * (rcv_parts - 1)
        + [jax.ShapeDtypeStruct(half, bf16)],
        [
            pltpu.VMEM((rcv_parts,) + piece, bf16),
            pltpu.VMEM(primaries.shape, f32),
            pltpu.VMEM(base.shape, f32),
            table,
            rows_half,
            pltpu.SemaphoreType.DMA((3, rcv_parts)),
        ],
        (me, *(pltpu.with_memory_space_constraint(array, pltpu.HBM) for array in (surface_operator, primaries, base))),
        2 * 1024 * 1024 * 256,
        [pltpu.SMEM] + [pltpu.HBM] * 3,
        [pltpu.VMEM] + [pltpu.HBM] * (rcv_parts - 1) + [pltpu.VMEM],
    )
    op = trade(op)
    tables = call(
        functools.partial(table_kernel, devices, rcv_parts),
        [pltpu.HBM((2 * NF, T_SIZE), bf16)] * 2,
        [table, pltpu.SemaphoreType.DMA((2,))],
        (base,),
        2**20,
        None,
        [pltpu.HBM] * 2,
    )
    for iteration in range(ITERS):
        points = exchange(spectra, devices)
        returned = rcv_parts if iteration + 1 == ITERS else 0
        packed, *residual = call(
            functools.partial(physics_kernel, rcv_parts, returned),
            [jax.ShapeDtypeStruct(wide, bf16)] + [pltpu.HBM((2, 2, rows, S), bf16)] * returned,
            [
                pltpu.VMEM((rcv_parts, 2, 2, rows, S), bf16),
                rows_half,
                rows_wide,
                pltpu.SemaphoreType.DMA((2, rcv_parts)),
            ],
            (points, *op, *data),
            4 * 2 * 768 * 512 * 256,
            [pltpu.VMEM] * (1 + 2 * rcv_parts),
            [pltpu.VMEM] + [pltpu.HBM] * returned,
        )
        packed = exchange(packed, devices)
        shape = pltpu.HBM(primaries.shape, f32)
        inputs = (packed, tables[iteration], pltpu.with_memory_space_constraint(primaries, pltpu.HBM), shrinkage)
        spaces = [pltpu.VMEM, pltpu.VMEM, pltpu.HBM, pltpu.VMEM]
        held = [rows_wide, pltpu.VMEM(primaries.shape, f32)]
        if iteration + 1 < ITERS:
            primaries, spectra = call(
                functools.partial(middle_kernel, devices),
                [shape, jax.ShapeDtypeStruct(half, bf16)],
                held + [rows_half, pltpu.SemaphoreType.DMA((2,))],
                inputs,
                4 * 1024 * 1024 * 256,
                spaces,
                [pltpu.HBM, pltpu.VMEM],
            )
        else:
            primaries, = call(
                functools.partial(last_kernel, devices),
                [shape],
                held + [pltpu.SemaphoreType.DMA((2,))],
                inputs,
                2 * 1024 * 1024 * 256,
                spaces,
                [pltpu.HBM],
            )
    residual = join(trade(residual), me)
    return (primaries, residual.transpose(2, 0, 1, 3))


def solution(mesh):
    freq_parts, rcv_parts = mesh.shape["freq"], mesh.shape["rcv"]

    def body(*args):
        return local(freq_parts, rcv_parts, *args)

    return jax.shard_map(
        body,
        mesh=mesh,
        in_specs=(
            P(("rcv", "freq"), None, None),
            P("freq", None, "rcv", None),
            P("rcv", "freq", None, None),
            P(),
        ),
        out_specs=(P(("rcv", "freq"), None, None), P("rcv", "freq", None, None)),
        check_vma=False,
    )
```

```python
import functools
import math

import jax
import jax.numpy as jnp
import numpy as np
from jax import lax
from jax.experimental import pallas as pl
from jax.experimental.pallas import tpu as pltpu
from jax.sharding import PartitionSpec as P


S = 128
NS = 512
R = 384
T_SIZE = 1024
ITERS = 2
NF = 512
ALL = ("rcv", "freq")
LANES = 128
EARLY = (4, 6, 2, 5, 7, 3, 1)
PARTS = 4
WIDE = PARTS + 1


def table_base(freq_parts, rcv_parts):
    freq_index = np.arange(NF).reshape(freq_parts, rcv_parts, -1).transpose(2, 1, 0).reshape(-1, 1)
    angle = freq_index * np.arange(LANES) % T_SIZE * (2.0 * math.pi / T_SIZE)
    factor = math.sqrt(2.0 / T_SIZE)
    return jnp.asarray(np.stack([factor * np.cos(angle), factor * np.sin(angle)]).astype(np.float32))


def fill_table(base_ref, table_ref, owners, rcv_parts):
    run = owners // rcv_parts
    for place in range(2):
        for owner in range(rcv_parts):
            rows = pl.ds(place * owners + owner * run, run)
            cosine, sine = base_ref[0, rows, :], base_ref[1, rows, :]
            for tile in range(T_SIZE // LANES):
                turn = math.pi / 4 * ((2 * owner + place) * tile % 8)
                cos, sin = round(math.cos(turn), 12), round(math.sin(turn), 12)
                columns = pl.ds(tile * LANES, LANES)
                real = cosine * cos - sine * sin
                imag = -(sine * cos + cosine * sin)
                for part, value in ((0, real), (1, imag)):
                    table_ref[pl.ds((2 * place + part) * owners + owner * run, run), columns] = value.astype(jnp.bfloat16)


def call(kernel, out_shape, scratch, inputs, flops, spaces=None, out_spaces=None):
    return pl.pallas_call(
        kernel,
        out_shape=out_shape,
        in_specs=[pl.BlockSpec(memory_space=space) for space in spaces or [pltpu.VMEM] * len(inputs)],
        out_specs=[pl.BlockSpec(memory_space=space) for space in out_spaces or [pltpu.VMEM] * len(out_shape)],
        scratch_shapes=scratch,
        compiler_params=pltpu.CompilerParams(vmem_limit_bytes=32 * 2**20),
        cost_estimate=pl.CostEstimate(flops=flops, bytes_accessed=4 * 2**20, transcendentals=0),
    )(*inputs)


def transform(table_ref, low, rows_ref, spectra_ref, owners):
    for part in range(PARTS):
        block = jnp.dot(table_ref[pl.ds(part * owners, owners), :], low, preferred_element_type=jnp.float32)
        for point in range(2):
            rows_ref[pl.ds(point * PARTS + part, owners, stride=2 * PARTS), :] = block[:, point * S:(point + 1) * S]
    spectra_ref[...] = rows_ref[...].astype(jnp.bfloat16)


def start_kernel(owners, blocks, me_ref, op_ref, data_ref, primaries_ref, base_ref, *refs):
    pieces, spectra_ref = refs[:blocks], refs[blocks]
    op_held, data_held, data_rows, piece_held, traces_ref, angles_ref, table_ref, rows_ref, sem = refs[blocks + 1:]
    frequencies = 2 * blocks
    rows = data_ref.shape[0] // (2 * frequencies)
    part = PARTS * rows
    fetches = [
        pltpu.make_async_copy(source, target, sem.at[blocks + place])
        for place, (source, target) in enumerate(
            ((base_ref, angles_ref), (data_ref, data_held), (op_ref, op_held), (primaries_ref, traces_ref))
        )
    ]
    fetch_base, fetch_data, fetch_op, fetch_traces = fetches
    for fetch in fetches:
        fetch.start()
    fetch_base.wait()
    fill_table(angles_ref, table_ref, owners, blocks)
    fetch_data.wait()
    data_rows[...] = data_held[...].astype(jnp.float32)
    fetch_op.wait()
    stores = []
    for place in EARLY + (0,):
        owner = me_ref[0] ^ place
        target = piece_held.at[place] if place else pieces[0]
        block = op_held[pl.ds(2 * owner, 2)].reshape(part, NS)
        for tile in range(NS // LANES):
            target[pl.ds(tile * part, part), :] = block[:, tile * LANES:(tile + 1) * LANES]
        for row in range(PARTS):
            recorded = data_rows[pl.ds(PARTS * owner + row, rows, stride=2 * frequencies), :]
            target[pl.ds(NS // LANES * part + row * rows, rows), :] = recorded.astype(jnp.bfloat16)
        if place:
            stores.append(pltpu.make_async_copy(target, pieces[place], sem.at[place]))
            stores[-1].start()
    fetch_traces.wait()
    low = jnp.concatenate([traces_ref[0].astype(jnp.bfloat16), traces_ref[1].astype(jnp.bfloat16)], axis=1)
    transform(table_ref, low, rows_ref, spectra_ref, owners)
    for store in stores:
        store.wait()


def split_three(value):
    high = value.astype(jnp.bfloat16).astype(jnp.float32)
    rest = value - high
    middle = rest.astype(jnp.bfloat16).astype(jnp.float32)
    return [high, middle, rest - middle]


def physics_kernel(blocks, rows, points_ref, *refs):
    pieces = refs[:blocks]
    packed_ref, *residual_refs, rows_ref, wide_ref = refs[blocks:]
    part = PARTS * rows
    rows_ref[...] = points_ref[...].astype(jnp.float32)
    residual_sq = jnp.zeros((1, 1), jnp.float32)
    direction_sq = jnp.zeros((1, 1), jnp.float32)
    for k in range(2):
        spectra = jnp.concatenate(
            [rows_ref[pl.ds(2 * k + c, NS, stride=PARTS), :].astype(jnp.bfloat16) for c in range(2)], axis=1
        )
        op = jnp.concatenate(
            [
                jnp.concatenate(
                    [piece[pl.ds(tile * part + 2 * k * rows, 2 * rows), :] for tile in range(NS // LANES)], axis=1
                )
                for piece in pieces
            ],
            axis=0,
        )
        product = jnp.dot(op, spectra, preferred_element_type=jnp.float32).reshape(blocks, 2, rows, 2 * S)
        stacked = []
        for a in range(blocks):
            real = product[a, 0, :, :S] - product[a, 1, :, S:]
            imag = product[a, 0, :, S:] + product[a, 1, :, :S]
            recorded = [
                pieces[a][pl.ds(NS // LANES * part + (2 * k + c) * rows, rows), :] for c in range(2)
            ]
            real = (recorded[0].astype(jnp.float32) - real).astype(jnp.bfloat16)
            imag = (recorded[1].astype(jnp.float32) - imag).astype(jnp.bfloat16)
            for residual_ref in residual_refs:
                residual_ref[a, k, 0] = real
                residual_ref[a, k, 1] = imag
            wide_real = real.astype(jnp.float32)
            wide_imag = imag.astype(jnp.float32)
            residual_sq += jnp.sum(wide_real * wide_real + wide_imag * wide_imag, keepdims=True)
            stacked.append(jnp.concatenate([real, imag], axis=1))
            stacked.append(jnp.concatenate([imag, -real], axis=1))
        direction = lax.dot_general(
            op, jnp.concatenate(stacked, axis=0), (((0,), (0,)), ((), ())), preferred_element_type=jnp.float32
        )
        direction_sq += jnp.sum(direction * direction, keepdims=True)
        for c in range(2):
            wide_ref[pl.ds(2 * k + c, NS, stride=WIDE), :] = direction[:, c * S:(c + 1) * S]
    lane = lax.broadcasted_iota(jnp.int32, (8, S), 1)
    sums = jnp.zeros((8, S), jnp.float32)
    for place, piece in enumerate(split_three(residual_sq) + split_three(direction_sq)):
        sums = jnp.where(lane == place, piece, sums)
    wide_ref[pl.ds(PARTS, NS, stride=WIDE), :] = jnp.broadcast_to(sums[:1], (NS, S))
    packed_ref[...] = wide_ref[...].astype(jnp.bfloat16)


def update(owners, packed_ref, table_ref, held_ref, shrinkage_ref, wide_ref, fetch, finish):
    wide_ref[...] = packed_ref[...].astype(jnp.float32)
    totals = jnp.sum(wide_ref[pl.ds(PARTS, owners, stride=2 * WIDE), :], axis=0, keepdims=True)
    lane = lax.broadcasted_iota(jnp.int32, (1, S), 1)
    residual_norm = jnp.sum(jnp.where(lane < 3, totals, 0.0), axis=1, keepdims=True)
    direction_norm = jnp.sum(jnp.where((lane >= 3) & (lane < 6), totals, 0.0), axis=1, keepdims=True)
    step_size = 0.5 * residual_norm / (direction_norm + 1e-06)
    threshold = shrinkage_ref[...] * (step_size * jnp.sqrt(direction_norm / (2.0 * NF * NS * S)))
    sides = []
    for point in range(2):
        pieces = [
            wide_ref[pl.ds(point * WIDE + part, owners, stride=2 * WIDE), :].astype(jnp.bfloat16)
            for part in range(PARTS)
        ]
        sides.append(jnp.concatenate(pieces, axis=0))
    direction = jnp.concatenate(sides, axis=1)
    block = T_SIZE // 4
    for start in range(0, T_SIZE, block):
        change = lax.dot_general(
            table_ref[:, pl.ds(start, block)], direction, (((0,), (0,)), ((), ())), preferred_element_type=jnp.float32
        )
        if fetch and not start:
            fetch.wait()
        news = []
        for point in range(2):
            moved = held_ref[point, pl.ds(start, block), :] + step_size * change[:, point * S:(point + 1) * S]
            news.append(moved - jnp.clip(moved, -threshold, threshold))
        finish(pl.ds(start, block), news)


def middle_kernel(owners, packed_ref, table_ref, primaries_ref, shrinkage_ref, new_ref, spectra_ref, wide_ref, rows_ref):
    lows = []

    def finish(window, news):
        for point, new in enumerate(news):
            new_ref[point, window, :] = new
        lows.append(jnp.concatenate([new.astype(jnp.bfloat16) for new in news], axis=1))

    update(owners, packed_ref, table_ref, primaries_ref, shrinkage_ref, wide_ref, None, finish)
    transform(table_ref, jnp.concatenate(lows, axis=0), rows_ref, spectra_ref, owners)


def last_kernel(owners, packed_ref, table_ref, primaries_ref, shrinkage_ref, new_ref, wide_ref, held_ref, sem):
    fetch = pltpu.make_async_copy(primaries_ref, held_ref, sem.at[4])
    fetch.start()
    stores = []

    def finish(window, news):
        for point, new in enumerate(news):
            held_ref[point, window, :] = new
        part = (slice(None), window)
        stores.append(pltpu.make_async_copy(held_ref.at[part], new_ref.at[part], sem.at[len(stores)]))
        stores[-1].start()

    update(owners, packed_ref, table_ref, held_ref, shrinkage_ref, wide_ref, fetch, finish)
    for store in stores:
        store.wait()


def table_kernel(owners, rcv_parts, base_ref, first_ref, second_ref, table_ref, sem):
    fill_table(base_ref, table_ref, owners, rcv_parts)
    stores = [pltpu.make_async_copy(table_ref, whole, sem.at[i]) for i, whole in enumerate((first_ref, second_ref))]
    for store in stores:
        store.start()
    for store in stores:
        store.wait()


def hand_out_kernel(whole_ref, *refs):
    *pieces, sem = refs
    copies = [pltpu.make_async_copy(whole_ref.at[a], piece, sem.at[a]) for a, piece in enumerate(pieces)]
    for copy in copies:
        copy.start()
    for copy in copies:
        copy.wait()


def join_kernel(blocks, me_ref, *refs):
    pieces, whole_ref = refs[:blocks], refs[blocks]
    for place, piece in enumerate(pieces):
        whole_ref[pl.ds(2 * (me_ref[0] ^ place), 2)] = piece[...]


def join(pieces, me):
    blocks = len(pieces)
    shape = pieces[0].shape
    return pl.pallas_call(
        functools.partial(join_kernel, blocks),
        out_shape=jax.ShapeDtypeStruct((2 * blocks,) + shape[1:], pieces[0].dtype),
        in_specs=[pl.BlockSpec(memory_space=pltpu.SMEM)] + [pl.BlockSpec(memory_space=pltpu.VMEM)] * blocks,
        out_specs=pl.BlockSpec(memory_space=pltpu.VMEM),
        compiler_params=pltpu.CompilerParams(vmem_limit_bytes=8 * 2**20),
    )(me, *pieces)


def trade(pieces):
    blocks = len(pieces)
    traded = [pieces[0]]
    for place in range(1, blocks):
        traded.append(lax.ppermute(pieces[place], "rcv", [(source, source ^ place) for source in range(blocks)]))
    return traded


def exchange(array, devices):
    pairs = array.reshape(devices, array.shape[0] // (2 * devices), 2, S)
    return lax.all_to_all(pairs, ALL, split_axis=0, concat_axis=0, tiled=True).reshape(array.shape)


def local(freq_parts, rcv_parts, primaries_start, surface_operator, data_spectra, shrinkage):
    devices = freq_parts * rcv_parts
    rows = R // rcv_parts
    half, wide = (devices * 2 * PARTS, S), (devices * 2 * WIDE, S)
    bf16, f32 = jnp.bfloat16, jnp.float32
    rows_half, rows_wide = pltpu.VMEM(half, f32), pltpu.VMEM(wide, f32)
    table = pltpu.VMEM((2 * NF, T_SIZE), bf16)
    base = table_base(freq_parts, rcv_parts)
    shrinkage = shrinkage.reshape(1, S)
    me = lax.axis_index("rcv").astype(jnp.int32).reshape(1)
    primaries = primaries_start
    piece = (PARTS * rows * (NS // LANES + 1), LANES)
    recorded = data_spectra.reshape(-1, S)
    arrays = (surface_operator, recorded, primaries, base)
    *pieces, spectra = call(
        functools.partial(start_kernel, devices, rcv_parts),
        [jax.ShapeDtypeStruct(piece, bf16)]
        + [pltpu.HBM(piece, bf16)] * (rcv_parts - 1)
        + [jax.ShapeDtypeStruct(half, bf16)],
        [
            pltpu.VMEM(surface_operator.shape, bf16),
            pltpu.VMEM(recorded.shape, bf16),
            pltpu.VMEM(recorded.shape, f32),
            pltpu.VMEM((rcv_parts,) + piece, bf16),
            pltpu.VMEM(primaries.shape, f32),
            pltpu.VMEM(base.shape, f32),
            table,
            rows_half,
            pltpu.SemaphoreType.DMA((rcv_parts + 4,)),
        ],
        (me, *(pltpu.with_memory_space_constraint(array, pltpu.HBM) for array in arrays)),
        2 * 1024 * 1024 * 256,
        [pltpu.SMEM] + [pltpu.HBM] * 4,
        [pltpu.VMEM] + [pltpu.HBM] * (rcv_parts - 1) + [pltpu.VMEM],
    )
    pieces = trade(pieces)
    tables = call(
        functools.partial(table_kernel, devices, rcv_parts),
        [pltpu.HBM((2 * NF, T_SIZE), bf16)] * 2,
        [table, pltpu.SemaphoreType.DMA((2,))],
        (base,),
        2**20,
        None,
        [pltpu.HBM] * 2,
    )
    for iteration in range(ITERS):
        points = exchange(spectra, devices)
        packed, *residual = call(
            functools.partial(physics_kernel, rcv_parts, rows),
            [jax.ShapeDtypeStruct(wide, bf16)]
            + [jax.ShapeDtypeStruct((rcv_parts, 2, 2, rows, S), bf16)] * (iteration + 1 == ITERS),
            [rows_half, rows_wide],
            (points, *pieces),
            4 * 2 * 768 * 512 * 256,
        )
        packed = exchange(packed, devices)
        if iteration + 1 < ITERS:
            primaries, spectra = call(
                functools.partial(middle_kernel, devices),
                [jax.ShapeDtypeStruct(primaries.shape, f32), jax.ShapeDtypeStruct(half, bf16)],
                [rows_wide, rows_half],
                (packed, tables[iteration], primaries, shrinkage),
                4 * 1024 * 1024 * 256,
            )
        else:
            primaries, = call(
                functools.partial(last_kernel, devices),
                [pltpu.HBM(primaries.shape, f32)],
                [rows_wide, pltpu.VMEM(primaries.shape, f32), pltpu.SemaphoreType.DMA((5,))],
                (packed, tables[iteration], pltpu.with_memory_space_constraint(primaries, pltpu.HBM), shrinkage),
                2 * 1024 * 1024 * 256,
                [pltpu.VMEM, pltpu.VMEM, pltpu.HBM, pltpu.VMEM],
                [pltpu.HBM],
            )
    residual, = residual
    residual = call(
        hand_out_kernel,
        [pltpu.HBM(residual.shape[1:], bf16)] * rcv_parts,
        [pltpu.SemaphoreType.DMA((rcv_parts,))],
        (residual,),
        2**20,
        None,
        [pltpu.HBM] * rcv_parts,
    )
    residual = join(trade(residual), me)
    return (primaries, residual.transpose(2, 0, 1, 3))


def solution(mesh):
    freq_parts, rcv_parts = mesh.shape["freq"], mesh.shape["rcv"]

    def body(*args):
        return local(freq_parts, rcv_parts, *args)

    return jax.shard_map(
        body,
        mesh=mesh,
        in_specs=(
            P(("rcv", "freq"), None, None),
            P("freq", None, "rcv", None),
            P("rcv", "freq", None, None),
            P(),
        ),
        out_specs=(P(("rcv", "freq"), None, None), P("rcv", "freq", None, None)),
        check_vma=False,
    )
```

```python
import functools
import math

import jax
import jax.numpy as jnp
import numpy as np
from jax import lax
from jax.experimental import pallas as pl
from jax.experimental.pallas import tpu as pltpu
from jax.sharding import PartitionSpec as P


S = 128
NS = 512
R = 384
T_SIZE = 1024
ITERS = 2
NF = 512
ALL = ("rcv", "freq")
LANES = 128
EARLY = (4, 6, 2, 5, 7, 3, 1)
PARTS = 4
WIDE = PARTS + 1


def table_base(freq_parts, rcv_parts):
    freq_index = np.arange(NF).reshape(freq_parts, rcv_parts, -1).transpose(2, 1, 0).reshape(-1, 1)
    angle = freq_index * np.arange(LANES) % T_SIZE * (2.0 * math.pi / T_SIZE)
    factor = math.sqrt(2.0 / T_SIZE)
    return jnp.asarray(np.stack([factor * np.cos(angle), factor * np.sin(angle)]).astype(np.float32))


def fill_table(base_ref, table_ref, owners, rcv_parts):
    run = owners // rcv_parts
    for place in range(2):
        for owner in range(rcv_parts):
            rows = pl.ds(place * owners + owner * run, run)
            cosine, sine = base_ref[0, rows, :], base_ref[1, rows, :]
            for tile in range(T_SIZE // LANES):
                turn = math.pi / 4 * ((2 * owner + place) * tile % 8)
                cos, sin = round(math.cos(turn), 12), round(math.sin(turn), 12)
                columns = pl.ds(tile * LANES, LANES)
                real = cosine * cos - sine * sin
                imag = -(sine * cos + cosine * sin)
                for part, value in ((0, real), (1, imag)):
                    table_ref[pl.ds((2 * place + part) * owners + owner * run, run), columns] = value.astype(jnp.bfloat16)


def call(kernel, out_shape, scratch, inputs, flops, spaces=None, out_spaces=None):
    return pl.pallas_call(
        kernel,
        out_shape=out_shape,
        in_specs=[pl.BlockSpec(memory_space=space) for space in spaces or [pltpu.VMEM] * len(inputs)],
        out_specs=[pl.BlockSpec(memory_space=space) for space in out_spaces or [pltpu.VMEM] * len(out_shape)],
        scratch_shapes=scratch,
        compiler_params=pltpu.CompilerParams(vmem_limit_bytes=32 * 2**20),
        cost_estimate=pl.CostEstimate(flops=flops, bytes_accessed=4 * 2**20, transcendentals=0),
    )(*inputs)


def transform(table_ref, low, rows_ref, spectra_ref, owners):
    for part in range(PARTS):
        block = jnp.dot(table_ref[pl.ds(part * owners, owners), :], low, preferred_element_type=jnp.float32)
        for point in range(2):
            rows_ref[pl.ds(point * PARTS + part, owners, stride=2 * PARTS), :] = block[:, point * S:(point + 1) * S]
    spectra_ref[...] = rows_ref[...].astype(jnp.bfloat16)


def start_kernel(owners, blocks, me_ref, op_ref, data_ref, primaries_ref, base_ref, *refs):
    pieces, spectra_ref = refs[:blocks], refs[blocks]
    op_held, data_held, data_rows, piece_held, traces_ref, angles_ref, table_ref, rows_ref, low_ref, sem = refs[blocks + 1:]
    frequencies = 2 * blocks
    rows = data_ref.shape[0] // (2 * frequencies)
    part = PARTS * rows
    fetches = [
        pltpu.make_async_copy(source, target, sem.at[blocks + place])
        for place, (source, target) in enumerate(
            ((base_ref, angles_ref), (primaries_ref, traces_ref), (data_ref, data_held), (op_ref, op_held))
        )
    ]
    fetch_base, fetch_traces, fetch_data, fetch_op = fetches
    for fetch in fetches:
        fetch.start()
    fetch_base.wait()
    fill_table(angles_ref, table_ref, owners, blocks)
    fetch_traces.wait()
    low = jnp.concatenate([traces_ref[0].astype(jnp.bfloat16), traces_ref[1].astype(jnp.bfloat16)], axis=1)
    transform(table_ref, low, rows_ref, low_ref, owners)
    stores = [pltpu.make_async_copy(low_ref, spectra_ref, sem.at[0])]
    stores[0].start()
    fetch_data.wait()
    data_rows[...] = data_held[...].astype(jnp.float32)
    fetch_op.wait()
    for place in EARLY + (0,):
        owner = me_ref[0] ^ place
        target = piece_held.at[place] if place else pieces[0]
        block = op_held[pl.ds(2 * owner, 2)].reshape(part, NS)
        for tile in range(NS // LANES):
            target[pl.ds(tile * part, part), :] = block[:, tile * LANES:(tile + 1) * LANES]
        for row in range(PARTS):
            recorded = data_rows[pl.ds(PARTS * owner + row, rows, stride=2 * frequencies), :]
            target[pl.ds(NS // LANES * part + row * rows, rows), :] = recorded.astype(jnp.bfloat16)
        if place:
            stores.append(pltpu.make_async_copy(target, pieces[place], sem.at[place]))
            stores[-1].start()
    for store in stores:
        store.wait()


def split_three(value):
    high = value.astype(jnp.bfloat16).astype(jnp.float32)
    rest = value - high
    middle = rest.astype(jnp.bfloat16).astype(jnp.float32)
    return [high, middle, rest - middle]


def physics_kernel(blocks, rows, points_ref, *refs):
    pieces = refs[:blocks]
    packed_ref, *residual_refs, rows_ref, wide_ref = refs[blocks:]
    part = PARTS * rows
    rows_ref[...] = points_ref[...].astype(jnp.float32)
    residual_sq = jnp.zeros((1, 1), jnp.float32)
    direction_sq = jnp.zeros((1, 1), jnp.float32)
    for k in range(2):
        spectra = jnp.concatenate(
            [rows_ref[pl.ds(2 * k + c, NS, stride=PARTS), :].astype(jnp.bfloat16) for c in range(2)], axis=1
        )
        op = jnp.concatenate(
            [
                jnp.concatenate(
                    [piece[pl.ds(tile * part + 2 * k * rows, 2 * rows), :] for tile in range(NS // LANES)], axis=1
                )
                for piece in pieces
            ],
            axis=0,
        )
        product = jnp.dot(op, spectra, preferred_element_type=jnp.float32).reshape(blocks, 2, rows, 2 * S)
        stacked = []
        for a in range(blocks):
            real = product[a, 0, :, :S] - product[a, 1, :, S:]
            imag = product[a, 0, :, S:] + product[a, 1, :, :S]
            recorded = [
                pieces[a][pl.ds(NS // LANES * part + (2 * k + c) * rows, rows), :] for c in range(2)
            ]
            real = (recorded[0].astype(jnp.float32) - real).astype(jnp.bfloat16)
            imag = (recorded[1].astype(jnp.float32) - imag).astype(jnp.bfloat16)
            for residual_ref in residual_refs:
                residual_ref[a, k, 0] = real
                residual_ref[a, k, 1] = imag
            wide_real = real.astype(jnp.float32)
            wide_imag = imag.astype(jnp.float32)
            residual_sq += jnp.sum(wide_real * wide_real + wide_imag * wide_imag, keepdims=True)
            stacked.append(jnp.concatenate([real, imag], axis=1))
            stacked.append(jnp.concatenate([imag, -real], axis=1))
        direction = lax.dot_general(
            op, jnp.concatenate(stacked, axis=0), (((0,), (0,)), ((), ())), preferred_element_type=jnp.float32
        )
        direction_sq += jnp.sum(direction * direction, keepdims=True)
        for c in range(2):
            wide_ref[pl.ds(2 * k + c, NS, stride=WIDE), :] = direction[:, c * S:(c + 1) * S]
    lane = lax.broadcasted_iota(jnp.int32, (8, S), 1)
    sums = jnp.zeros((8, S), jnp.float32)
    for place, piece in enumerate(split_three(residual_sq) + split_three(direction_sq)):
        sums = jnp.where(lane == place, piece, sums)
    wide_ref[pl.ds(PARTS, NS, stride=WIDE), :] = jnp.broadcast_to(sums[:1], (NS, S))
    packed_ref[...] = wide_ref[...].astype(jnp.bfloat16)


def update(owners, packed_ref, table_ref, held_ref, shrinkage_ref, wide_ref, fetch, finish):
    wide_ref[...] = packed_ref[...].astype(jnp.float32)
    totals = jnp.sum(wide_ref[pl.ds(PARTS, owners, stride=2 * WIDE), :], axis=0, keepdims=True)
    lane = lax.broadcasted_iota(jnp.int32, (1, S), 1)
    residual_norm = jnp.sum(jnp.where(lane < 3, totals, 0.0), axis=1, keepdims=True)
    direction_norm = jnp.sum(jnp.where((lane >= 3) & (lane < 6), totals, 0.0), axis=1, keepdims=True)
    step_size = 0.5 * residual_norm / (direction_norm + 1e-06)
    threshold = shrinkage_ref[...] * (step_size * jnp.sqrt(direction_norm / (2.0 * NF * NS * S)))
    sides = []
    for point in range(2):
        pieces = [
            wide_ref[pl.ds(point * WIDE + part, owners, stride=2 * WIDE), :].astype(jnp.bfloat16)
            for part in range(PARTS)
        ]
        sides.append(jnp.concatenate(pieces, axis=0))
    direction = jnp.concatenate(sides, axis=1)
    block = T_SIZE // 4
    changes = [
        lax.dot_general(
            table_ref[:, pl.ds(start, block)], direction, (((0,), (0,)), ((), ())), preferred_element_type=jnp.float32
        )
        for start in range(0, T_SIZE, block)
    ]
    if fetch:
        fetch.wait()
    for start, change in zip(range(0, T_SIZE, block), changes):
        news = []
        for point in range(2):
            moved = held_ref[point, pl.ds(start, block), :] + step_size * change[:, point * S:(point + 1) * S]
            news.append(moved - jnp.clip(moved, -threshold, threshold))
        finish(pl.ds(start, block), news)


def middle_kernel(owners, packed_ref, table_ref, primaries_ref, shrinkage_ref, new_ref, spectra_ref, wide_ref, rows_ref):
    lows = []

    def finish(window, news):
        for point, new in enumerate(news):
            new_ref[point, window, :] = new
        lows.append(jnp.concatenate([new.astype(jnp.bfloat16) for new in news], axis=1))

    update(owners, packed_ref, table_ref, primaries_ref, shrinkage_ref, wide_ref, None, finish)
    transform(table_ref, jnp.concatenate(lows, axis=0), rows_ref, spectra_ref, owners)


def last_kernel(owners, packed_ref, table_ref, primaries_ref, shrinkage_ref, new_ref, wide_ref, held_ref, sem):
    fetch = pltpu.make_async_copy(primaries_ref, held_ref, sem.at[4])
    fetch.start()
    stores = []

    def finish(window, news):
        for point, new in enumerate(news):
            held_ref[point, window, :] = new
        part = (slice(None), window)
        stores.append(pltpu.make_async_copy(held_ref.at[part], new_ref.at[part], sem.at[len(stores)]))
        stores[-1].start()

    update(owners, packed_ref, table_ref, held_ref, shrinkage_ref, wide_ref, fetch, finish)
    for store in stores:
        store.wait()


def table_kernel(owners, rcv_parts, base_ref, first_ref, second_ref, table_ref, sem):
    fill_table(base_ref, table_ref, owners, rcv_parts)
    stores = [pltpu.make_async_copy(table_ref, whole, sem.at[i]) for i, whole in enumerate((first_ref, second_ref))]
    for store in stores:
        store.start()
    for store in stores:
        store.wait()


def hand_out_kernel(whole_ref, *refs):
    *pieces, sem = refs
    copies = [pltpu.make_async_copy(whole_ref.at[a], piece, sem.at[a]) for a, piece in enumerate(pieces)]
    for copy in copies:
        copy.start()
    for copy in copies:
        copy.wait()


def join_kernel(blocks, me_ref, *refs):
    pieces, whole_ref = refs[:blocks], refs[blocks]
    for place, piece in enumerate(pieces):
        whole_ref[pl.ds(2 * (me_ref[0] ^ place), 2)] = piece[...]


def join(pieces, me):
    blocks = len(pieces)
    shape = pieces[0].shape
    return pl.pallas_call(
        functools.partial(join_kernel, blocks),
        out_shape=jax.ShapeDtypeStruct((2 * blocks,) + shape[1:], pieces[0].dtype),
        in_specs=[pl.BlockSpec(memory_space=pltpu.SMEM)] + [pl.BlockSpec(memory_space=pltpu.VMEM)] * blocks,
        out_specs=pl.BlockSpec(memory_space=pltpu.VMEM),
        compiler_params=pltpu.CompilerParams(vmem_limit_bytes=8 * 2**20),
    )(me, *pieces)


def trade(pieces):
    blocks = len(pieces)
    traded = [pieces[0]]
    for place in range(1, blocks):
        traded.append(lax.ppermute(pieces[place], "rcv", [(source, source ^ place) for source in range(blocks)]))
    return traded


def exchange(array, devices):
    pairs = array.reshape(devices, array.shape[0] // (2 * devices), 2, S)
    return lax.all_to_all(pairs, ALL, split_axis=0, concat_axis=0, tiled=True).reshape(array.shape)


def local(freq_parts, rcv_parts, primaries_start, surface_operator, data_spectra, shrinkage):
    devices = freq_parts * rcv_parts
    rows = R // rcv_parts
    half, wide = (devices * 2 * PARTS, S), (devices * 2 * WIDE, S)
    bf16, f32 = jnp.bfloat16, jnp.float32
    rows_half, rows_wide = pltpu.VMEM(half, f32), pltpu.VMEM(wide, f32)
    table = pltpu.VMEM((2 * NF, T_SIZE), bf16)
    base = table_base(freq_parts, rcv_parts)
    shrinkage = shrinkage.reshape(1, S)
    me = lax.axis_index("rcv").astype(jnp.int32).reshape(1)
    primaries = primaries_start
    piece = (PARTS * rows * (NS // LANES + 1), LANES)
    recorded = data_spectra.reshape(-1, S)
    arrays = (surface_operator, recorded, primaries, base)
    *pieces, spectra = call(
        functools.partial(start_kernel, devices, rcv_parts),
        [jax.ShapeDtypeStruct(piece, bf16)]
        + [pltpu.HBM(piece, bf16)] * (rcv_parts - 1)
        + [pltpu.HBM(half, bf16)],
        [
            pltpu.VMEM(surface_operator.shape, bf16),
            pltpu.VMEM(recorded.shape, bf16),
            pltpu.VMEM(recorded.shape, f32),
            pltpu.VMEM((rcv_parts,) + piece, bf16),
            pltpu.VMEM(primaries.shape, f32),
            pltpu.VMEM(base.shape, f32),
            table,
            rows_half,
            pltpu.VMEM(half, bf16),
            pltpu.SemaphoreType.DMA((rcv_parts + 4,)),
        ],
        (me, *(pltpu.with_memory_space_constraint(array, pltpu.HBM) for array in arrays)),
        2 * 1024 * 1024 * 256,
        [pltpu.SMEM] + [pltpu.HBM] * 4,
        [pltpu.VMEM] + [pltpu.HBM] * rcv_parts,
    )
    pieces = trade(pieces)
    tables = call(
        functools.partial(table_kernel, devices, rcv_parts),
        [pltpu.HBM((2 * NF, T_SIZE), bf16)] * 2,
        [table, pltpu.SemaphoreType.DMA((2,))],
        (base,),
        2**20,
        None,
        [pltpu.HBM] * 2,
    )
    for iteration in range(ITERS):
        points = exchange(spectra, devices)
        packed, *residual = call(
            functools.partial(physics_kernel, rcv_parts, rows),
            [jax.ShapeDtypeStruct(wide, bf16)]
            + [jax.ShapeDtypeStruct((rcv_parts, 2, 2, rows, S), bf16)] * (iteration + 1 == ITERS),
            [rows_half, rows_wide],
            (points, *pieces),
            4 * 2 * 768 * 512 * 256,
        )
        packed = exchange(packed, devices)
        if iteration + 1 < ITERS:
            primaries, spectra = call(
                functools.partial(middle_kernel, devices),
                [jax.ShapeDtypeStruct(primaries.shape, f32), jax.ShapeDtypeStruct(half, bf16)],
                [rows_wide, rows_half],
                (packed, tables[iteration], primaries, shrinkage),
                4 * 1024 * 1024 * 256,
            )
        else:
            primaries, = call(
                functools.partial(last_kernel, devices),
                [pltpu.HBM(primaries.shape, f32)],
                [rows_wide, pltpu.VMEM(primaries.shape, f32), pltpu.SemaphoreType.DMA((5,))],
                (packed, tables[iteration], pltpu.with_memory_space_constraint(primaries, pltpu.HBM), shrinkage),
                2 * 1024 * 1024 * 256,
                [pltpu.VMEM, pltpu.VMEM, pltpu.HBM, pltpu.VMEM],
                [pltpu.HBM],
            )
    residual, = residual
    residual = call(
        hand_out_kernel,
        [pltpu.HBM(residual.shape[1:], bf16)] * rcv_parts,
        [pltpu.SemaphoreType.DMA((rcv_parts,))],
        (residual,),
        2**20,
        None,
        [pltpu.HBM] * rcv_parts,
    )
    residual = join(trade(residual), me)
    return (primaries, residual.transpose(2, 0, 1, 3))


def solution(mesh):
    freq_parts, rcv_parts = mesh.shape["freq"], mesh.shape["rcv"]

    def body(*args):
        return local(freq_parts, rcv_parts, *args)

    return jax.shard_map(
        body,
        mesh=mesh,
        in_specs=(
            P(("rcv", "freq"), None, None),
            P("freq", None, "rcv", None),
            P("rcv", "freq", None, None),
            P(),
        ),
        out_specs=(P(("rcv", "freq"), None, None), P("rcv", "freq", None, None)),
        check_vma=False,
    )
```

```python
import functools
import math

import jax
import jax.numpy as jnp
import numpy as np
from jax import lax
from jax.experimental import pallas as pl
from jax.experimental.pallas import tpu as pltpu
from jax.sharding import PartitionSpec as P


S = 128
NS = 512
R = 384
T_SIZE = 1024
ITERS = 2
NF = 512
ALL = ("rcv", "freq")
LANES = 128
EARLY = (4, 6, 2, 5, 7, 3, 1)
PARTS = 4
WIDE = PARTS + 1


def table_base(freq_parts, rcv_parts):
    freq_index = np.arange(NF).reshape(freq_parts, rcv_parts, -1).transpose(2, 1, 0).reshape(-1, 1)
    angle = freq_index * np.arange(LANES) % T_SIZE * (2.0 * math.pi / T_SIZE)
    factor = math.sqrt(2.0 / T_SIZE)
    return jnp.asarray(np.stack([factor * np.cos(angle), factor * np.sin(angle)]).astype(np.float32))


def fill_table(base_ref, table_ref, owners, rcv_parts):
    run = owners // rcv_parts
    for place in range(2):
        for owner in range(rcv_parts):
            rows = pl.ds(place * owners + owner * run, run)
            cosine, sine = base_ref[0, rows, :], base_ref[1, rows, :]
            for tile in range(T_SIZE // LANES):
                turn = math.pi / 4 * ((2 * owner + place) * tile % 8)
                cos, sin = round(math.cos(turn), 12), round(math.sin(turn), 12)
                columns = pl.ds(tile * LANES, LANES)
                real = cosine * cos - sine * sin
                imag = -(sine * cos + cosine * sin)
                for part, value in ((0, real), (1, imag)):
                    table_ref[pl.ds((2 * place + part) * owners + owner * run, run), columns] = value.astype(jnp.bfloat16)


def call(kernel, out_shape, scratch, inputs, flops, spaces=None, out_spaces=None):
    return pl.pallas_call(
        kernel,
        out_shape=out_shape,
        in_specs=[pl.BlockSpec(memory_space=space) for space in spaces or [pltpu.VMEM] * len(inputs)],
        out_specs=[pl.BlockSpec(memory_space=space) for space in out_spaces or [pltpu.VMEM] * len(out_shape)],
        scratch_shapes=scratch,
        compiler_params=pltpu.CompilerParams(vmem_limit_bytes=32 * 2**20),
        cost_estimate=pl.CostEstimate(flops=flops, bytes_accessed=4 * 2**20, transcendentals=0),
    )(*inputs)


def transform(table_ref, low, rows_ref, spectra_ref, owners):
    for part in range(PARTS):
        block = jnp.dot(table_ref[pl.ds(part * owners, owners), :], low, preferred_element_type=jnp.float32)
        for point in range(2):
            rows_ref[pl.ds(point * PARTS + part, owners, stride=2 * PARTS), :] = block[:, point * S:(point + 1) * S]
    spectra_ref[...] = rows_ref[...].astype(jnp.bfloat16)


def start_kernel(owners, blocks, me_ref, op_ref, data_ref, primaries_ref, base_ref, *refs):
    pieces, spectra_ref = refs[:blocks], refs[blocks]
    op_held, data_held, data_rows, piece_held, traces_ref, angles_ref, table_ref, rows_ref, low_ref, sem = refs[blocks + 1:]
    frequencies = 2 * blocks
    rows = data_ref.shape[0] // (2 * frequencies)
    part = PARTS * rows
    fetches = [
        pltpu.make_async_copy(source, target, sem.at[blocks + place])
        for place, (source, target) in enumerate(
            ((base_ref, angles_ref), (primaries_ref, traces_ref), (data_ref, data_held), (op_ref, op_held))
        )
    ]
    fetch_base, fetch_traces, fetch_data, fetch_op = fetches
    for fetch in fetches:
        fetch.start()
    fetch_base.wait()
    fill_table(angles_ref, table_ref, owners, blocks)
    fetch_traces.wait()
    low = jnp.concatenate([traces_ref[0].astype(jnp.bfloat16), traces_ref[1].astype(jnp.bfloat16)], axis=1)
    transform(table_ref, low, rows_ref, low_ref, owners)
    stores = [pltpu.make_async_copy(low_ref, spectra_ref, sem.at[0])]
    stores[0].start()
    fetch_data.wait()
    data_rows[...] = data_held[...].astype(jnp.float32)
    fetch_op.wait()
    for place in EARLY + (0,):
        owner = me_ref[0] ^ place
        target = piece_held.at[place] if place else pieces[0]
        block = op_held[pl.ds(2 * owner, 2)].reshape(part, NS)
        for tile in range(NS // LANES):
            target[pl.ds(tile * part, part), :] = block[:, tile * LANES:(tile + 1) * LANES]
        for row in range(PARTS):
            recorded = data_rows[pl.ds(PARTS * owner + row, rows, stride=2 * frequencies), :]
            target[pl.ds(NS // LANES * part + row * rows, rows), :] = recorded.astype(jnp.bfloat16)
        if place:
            stores.append(pltpu.make_async_copy(target, pieces[place], sem.at[place]))
            stores[-1].start()
    for store in stores:
        store.wait()


def split_three(value):
    high = value.astype(jnp.bfloat16).astype(jnp.float32)
    rest = value - high
    middle = rest.astype(jnp.bfloat16).astype(jnp.float32)
    return [high, middle, rest - middle]


def physics_kernel(blocks, rows, points_ref, *refs):
    pieces = refs[:blocks]
    packed_ref, *residual_refs, rows_ref, wide_ref = refs[blocks:]
    part = PARTS * rows
    rows_ref[...] = points_ref[...].astype(jnp.float32)
    residual_sq = jnp.zeros((1, 1), jnp.float32)
    direction_sq = jnp.zeros((1, 1), jnp.float32)
    ops, products, resids = [], [], []
    for k in range(2):
        spectra = jnp.concatenate(
            [rows_ref[pl.ds(2 * k + c, NS, stride=PARTS), :].astype(jnp.bfloat16) for c in range(2)], axis=1
        )
        op = jnp.concatenate(
            [
                jnp.concatenate(
                    [piece[pl.ds(tile * part + 2 * k * rows, 2 * rows), :] for tile in range(NS // LANES)], axis=1
                )
                for piece in pieces
            ],
            axis=0,
        )
        product = jnp.dot(op, spectra, preferred_element_type=jnp.float32).reshape(blocks, 2, rows, 2 * S)
        ops.append(op)
        products.append(product)
    for k, product in enumerate(products):
        stacked = []
        for a in range(blocks):
            real = product[a, 0, :, :S] - product[a, 1, :, S:]
            imag = product[a, 0, :, S:] + product[a, 1, :, :S]
            recorded = [
                pieces[a][pl.ds(NS // LANES * part + (2 * k + c) * rows, rows), :] for c in range(2)
            ]
            real = (recorded[0].astype(jnp.float32) - real).astype(jnp.bfloat16)
            imag = (recorded[1].astype(jnp.float32) - imag).astype(jnp.bfloat16)
            for residual_ref in residual_refs:
                residual_ref[a, k, 0] = real
                residual_ref[a, k, 1] = imag
            wide_real = real.astype(jnp.float32)
            wide_imag = imag.astype(jnp.float32)
            residual_sq += jnp.sum(wide_real * wide_real + wide_imag * wide_imag, keepdims=True)
            stacked.append(jnp.concatenate([real, imag], axis=1))
            stacked.append(jnp.concatenate([imag, -real], axis=1))
        resids.append(jnp.concatenate(stacked, axis=0))
    for k in range(2):
        direction = lax.dot_general(
            ops[k], resids[k], (((0,), (0,)), ((), ())), preferred_element_type=jnp.float32
        )
        direction_sq += jnp.sum(direction * direction, keepdims=True)
        for c in range(2):
            wide_ref[pl.ds(2 * k + c, NS, stride=WIDE), :] = direction[:, c * S:(c + 1) * S]
    lane = lax.broadcasted_iota(jnp.int32, (8, S), 1)
    sums = jnp.zeros((8, S), jnp.float32)
    for place, piece in enumerate(split_three(residual_sq) + split_three(direction_sq)):
        sums = jnp.where(lane == place, piece, sums)
    wide_ref[pl.ds(PARTS, NS, stride=WIDE), :] = jnp.broadcast_to(sums[:1], (NS, S))
    packed_ref[...] = wide_ref[...].astype(jnp.bfloat16)


def update(owners, packed_ref, table_ref, held_ref, shrinkage_ref, wide_ref, fetch, finish):
    wide_ref[...] = packed_ref[...].astype(jnp.float32)
    totals = jnp.sum(wide_ref[pl.ds(PARTS, owners, stride=2 * WIDE), :], axis=0, keepdims=True)
    lane = lax.broadcasted_iota(jnp.int32, (1, S), 1)
    residual_norm = jnp.sum(jnp.where(lane < 3, totals, 0.0), axis=1, keepdims=True)
    direction_norm = jnp.sum(jnp.where((lane >= 3) & (lane < 6), totals, 0.0), axis=1, keepdims=True)
    step_size = 0.5 * residual_norm / (direction_norm + 1e-06)
    threshold = shrinkage_ref[...] * (step_size * jnp.sqrt(direction_norm / (2.0 * NF * NS * S)))
    sides = []
    for point in range(2):
        pieces = [
            wide_ref[pl.ds(point * WIDE + part, owners, stride=2 * WIDE), :].astype(jnp.bfloat16)
            for part in range(PARTS)
        ]
        sides.append(jnp.concatenate(pieces, axis=0))
    direction = jnp.concatenate(sides, axis=1)
    block = T_SIZE // 4
    changes = [
        lax.dot_general(
            table_ref[:, pl.ds(start, block)], direction, (((0,), (0,)), ((), ())), preferred_element_type=jnp.float32
        )
        for start in range(0, T_SIZE, block)
    ]
    if fetch:
        fetch.wait()
    for start, change in zip(range(0, T_SIZE, block), changes):
        news = []
        for point in range(2):
            moved = held_ref[point, pl.ds(start, block), :] + step_size * change[:, point * S:(point + 1) * S]
            news.append(moved - jnp.clip(moved, -threshold, threshold))
        finish(pl.ds(start, block), news)


def middle_kernel(owners, packed_ref, table_ref, primaries_ref, shrinkage_ref, new_ref, spectra_ref, wide_ref, rows_ref):
    lows = []

    def finish(window, news):
        for point, new in enumerate(news):
            new_ref[point, window, :] = new
        lows.append(jnp.concatenate([new.astype(jnp.bfloat16) for new in news], axis=1))

    update(owners, packed_ref, table_ref, primaries_ref, shrinkage_ref, wide_ref, None, finish)
    transform(table_ref, jnp.concatenate(lows, axis=0), rows_ref, spectra_ref, owners)


def last_kernel(owners, packed_ref, table_ref, primaries_ref, shrinkage_ref, new_ref, wide_ref, held_ref, sem):
    fetch = pltpu.make_async_copy(primaries_ref, held_ref, sem.at[4])
    fetch.start()
    stores = []

    def finish(window, news):
        for point, new in enumerate(news):
            held_ref[point, window, :] = new
        part = (slice(None), window)
        stores.append(pltpu.make_async_copy(held_ref.at[part], new_ref.at[part], sem.at[len(stores)]))
        stores[-1].start()

    update(owners, packed_ref, table_ref, held_ref, shrinkage_ref, wide_ref, fetch, finish)
    for store in stores:
        store.wait()


def table_kernel(owners, rcv_parts, base_ref, first_ref, second_ref, table_ref, sem):
    fill_table(base_ref, table_ref, owners, rcv_parts)
    stores = [pltpu.make_async_copy(table_ref, whole, sem.at[i]) for i, whole in enumerate((first_ref, second_ref))]
    for store in stores:
        store.start()
    for store in stores:
        store.wait()


def hand_out_kernel(whole_ref, *refs):
    *pieces, sem = refs
    copies = [pltpu.make_async_copy(whole_ref.at[a], piece, sem.at[a]) for a, piece in enumerate(pieces)]
    for copy in copies:
        copy.start()
    for copy in copies:
        copy.wait()


def join_kernel(blocks, me_ref, *refs):
    pieces, whole_ref = refs[:blocks], refs[blocks]
    for place, piece in enumerate(pieces):
        whole_ref[pl.ds(2 * (me_ref[0] ^ place), 2)] = piece[...]


def join(pieces, me):
    blocks = len(pieces)
    shape = pieces[0].shape
    return pl.pallas_call(
        functools.partial(join_kernel, blocks),
        out_shape=jax.ShapeDtypeStruct((2 * blocks,) + shape[1:], pieces[0].dtype),
        in_specs=[pl.BlockSpec(memory_space=pltpu.SMEM)] + [pl.BlockSpec(memory_space=pltpu.VMEM)] * blocks,
        out_specs=pl.BlockSpec(memory_space=pltpu.VMEM),
        compiler_params=pltpu.CompilerParams(vmem_limit_bytes=8 * 2**20),
    )(me, *pieces)


def trade(pieces):
    blocks = len(pieces)
    traded = [pieces[0]]
    for place in range(1, blocks):
        traded.append(lax.ppermute(pieces[place], "rcv", [(source, source ^ place) for source in range(blocks)]))
    return traded


def exchange(array, devices):
    pairs = array.reshape(devices, array.shape[0] // (2 * devices), 2, S)
    return lax.all_to_all(pairs, ALL, split_axis=0, concat_axis=0, tiled=True).reshape(array.shape)


def local(freq_parts, rcv_parts, primaries_start, surface_operator, data_spectra, shrinkage):
    devices = freq_parts * rcv_parts
    rows = R // rcv_parts
    half, wide = (devices * 2 * PARTS, S), (devices * 2 * WIDE, S)
    bf16, f32 = jnp.bfloat16, jnp.float32
    rows_half, rows_wide = pltpu.VMEM(half, f32), pltpu.VMEM(wide, f32)
    table = pltpu.VMEM((2 * NF, T_SIZE), bf16)
    base = table_base(freq_parts, rcv_parts)
    shrinkage = shrinkage.reshape(1, S)
    me = lax.axis_index("rcv").astype(jnp.int32).reshape(1)
    primaries = primaries_start
    piece = (PARTS * rows * (NS // LANES + 1), LANES)
    recorded = data_spectra.reshape(-1, S)
    arrays = (surface_operator, recorded, primaries, base)
    *pieces, spectra = call(
        functools.partial(start_kernel, devices, rcv_parts),
        [jax.ShapeDtypeStruct(piece, bf16)]
        + [pltpu.HBM(piece, bf16)] * (rcv_parts - 1)
        + [pltpu.HBM(half, bf16)],
        [
            pltpu.VMEM(surface_operator.shape, bf16),
            pltpu.VMEM(recorded.shape, bf16),
            pltpu.VMEM(recorded.shape, f32),
            pltpu.VMEM((rcv_parts,) + piece, bf16),
            pltpu.VMEM(primaries.shape, f32),
            pltpu.VMEM(base.shape, f32),
            table,
            rows_half,
            pltpu.VMEM(half, bf16),
            pltpu.SemaphoreType.DMA((rcv_parts + 4,)),
        ],
        (me, *(pltpu.with_memory_space_constraint(array, pltpu.HBM) for array in arrays)),
        2 * 1024 * 1024 * 256,
        [pltpu.SMEM] + [pltpu.HBM] * 4,
        [pltpu.VMEM] + [pltpu.HBM] * rcv_parts,
    )
    pieces = trade(pieces)
    tables = call(
        functools.partial(table_kernel, devices, rcv_parts),
        [pltpu.HBM((2 * NF, T_SIZE), bf16)] * 2,
        [table, pltpu.SemaphoreType.DMA((2,))],
        (base,),
        2**20,
        None,
        [pltpu.HBM] * 2,
    )
    for iteration in range(ITERS):
        points = exchange(spectra, devices)
        packed, *residual = call(
            functools.partial(physics_kernel, rcv_parts, rows),
            [jax.ShapeDtypeStruct(wide, bf16)]
            + [jax.ShapeDtypeStruct((rcv_parts, 2, 2, rows, S), bf16)] * (iteration + 1 == ITERS),
            [rows_half, rows_wide],
            (points, *pieces),
            4 * 2 * 768 * 512 * 256,
        )
        packed = exchange(packed, devices)
        if iteration + 1 < ITERS:
            primaries, spectra = call(
                functools.partial(middle_kernel, devices),
                [jax.ShapeDtypeStruct(primaries.shape, f32), jax.ShapeDtypeStruct(half, bf16)],
                [rows_wide, rows_half],
                (packed, tables[iteration], primaries, shrinkage),
                4 * 1024 * 1024 * 256,
            )
        else:
            primaries, = call(
                functools.partial(last_kernel, devices),
                [pltpu.HBM(primaries.shape, f32)],
                [rows_wide, pltpu.VMEM(primaries.shape, f32), pltpu.SemaphoreType.DMA((5,))],
                (packed, tables[iteration], pltpu.with_memory_space_constraint(primaries, pltpu.HBM), shrinkage),
                2 * 1024 * 1024 * 256,
                [pltpu.VMEM, pltpu.VMEM, pltpu.HBM, pltpu.VMEM],
                [pltpu.HBM],
            )
    residual, = residual
    residual = call(
        hand_out_kernel,
        [pltpu.HBM(residual.shape[1:], bf16)] * rcv_parts,
        [pltpu.SemaphoreType.DMA((rcv_parts,))],
        (residual,),
        2**20,
        None,
        [pltpu.HBM] * rcv_parts,
    )
    residual = join(trade(residual), me)
    return (primaries, residual.transpose(2, 0, 1, 3))


def solution(mesh):
    freq_parts, rcv_parts = mesh.shape["freq"], mesh.shape["rcv"]

    def body(*args):
        return local(freq_parts, rcv_parts, *args)

    return jax.shard_map(
        body,
        mesh=mesh,
        in_specs=(
            P(("rcv", "freq"), None, None),
            P("freq", None, "rcv", None),
            P("rcv", "freq", None, None),
            P(),
        ),
        out_specs=(P(("rcv", "freq"), None, None), P("rcv", "freq", None, None)),
        check_vma=False,
    )
```
